512 devices in a mesh: grp: 8 (over z_lo, x), tile: 64 (over z_hi, y, core).
Axes of the slice: x: 4, y: 8, z: 8 (z_hi: 4, z_lo: 2; z = z_hi * 2 + z_lo), core: 2. Of those that a mesh axis runs over, the one named last changes fastest.
Arguments:
- quantized: bfloat16 [16, 384, 8192], P(None, 'grp', 'tile'), may hold values from -6 to 6
- scales: float32 [64, 16, 384], P('tile', None, 'grp'), may hold values from 0.25 to 4
Outputs:
- coefficients: bfloat16 [16, 384, 8192], P(None, 'grp', 'tile')
The draws below stay inside these ranges and needn't reach their ends.
All inputs are finite; a program needn't handle non-finite values.
Results may differ from the reference program's by a relative error of at most 0.001.
Values sent between devices are 32-bit elements; how exact they have to be, the bound alone decides.
A program may use at most 64 MiB of HBM per device.

```python
import math
import jax
import jax.numpy as jnp
from jax import lax

NZ = 16
QB = 128
LEVELS = 4
NY = 384
NX = 8192


def steps_of(rng, extent, pieces, low, top_value):
    def one(dim, parts):
        steps = jax.random.uniform(jax.random.fold_in(jax.random.fold_in(rng, 6), dim), (parts,), jnp.float32, low / len(pieces), top_value / len(pieces))
        return jnp.repeat(jnp.exp(steps), extent[dim] // parts).reshape((-1,) + (1,) * (len(extent) - dim - 1))

    factor_of = one(*pieces[0])
    for cut in pieces[1:]:
        factor_of = factor_of * one(*cut)
    return factor_of


def noise(own_key, dims, scale, limit, split=(), dtype=jnp.bfloat16):
    level = steps_of(own_key, dims, split, -0.22, 0.18) if split else 1.0
    array = jax.random.normal(own_key, dims, jnp.float32) * scale * level
    return jnp.minimum(jnp.maximum(array, -limit), limit).astype(dtype)


def setup_inputs(seed: int = 0) -> dict:
    splits = jax.random.split(jax.random.key(seed), 3)
    quantized = noise(splits[0], (NZ, NY, NX), 1.0, 6.0, ((1, 8), (2, 64)))
    scales = jnp.clip(jnp.exp(math.log(4.0) - 2.7725887 * jax.random.uniform(splits[1], (NX // QB, NZ, NY), jnp.float32) ** steps_of(splits[1], (NX // QB, NZ, NY), ((0, 64), (2, 8)), -0.2, 0.2)), 0.25, 4.0)
    return dict(quantized=quantized, scales=scales)


LIFT_ALPHA = -1.586134342059924
LIFT_BETA = -0.052980118572961
LIFT_GAMMA = 0.882911075530934
LIFT_DELTA = 0.443506852043971
LIFT_KAPPA = 1.230174104914001


def forward_of(values, along):
    length = values.shape[along]
    return jnp.concatenate([lax.slice_in_dim(values, 1, length, 1, along), lax.slice_in_dim(values, length - 1, length, 1, along)], along)


def backward_of(values, along):
    length = values.shape[along]
    return jnp.concatenate([lax.slice_in_dim(values, 0, 1, 1, along), lax.slice_in_dim(values, 0, length - 1, 1, along)], along)


def lift_axis(subband, along):
    length = subband.shape[along]
    even_part = lax.slice_in_dim(subband, 0, length, 2, along)
    odd_part = lax.slice_in_dim(subband, 1, length, 2, along)
    odd_part = odd_part + LIFT_ALPHA * (even_part + forward_of(even_part, along))
    even_part = even_part + LIFT_BETA * (backward_of(odd_part, along) + odd_part)
    odd_part = odd_part + LIFT_GAMMA * (even_part + forward_of(even_part, along))
    even_part = even_part + LIFT_DELTA * (backward_of(odd_part, along) + odd_part)
    even_part = even_part / LIFT_KAPPA
    odd_part = odd_part * (LIFT_KAPPA / 2.0)
    return jnp.stack([even_part, odd_part], along + 1).reshape(subband.shape)


def decompose(subband, level_index):
    for along in (2, 1, 0):
        subband = lift_axis(subband, along)
    if level_index + 1 < LEVELS:
        coarser = decompose(subband[::2, ::2, ::2], level_index + 1)
        subband = subband.at[::2, ::2, ::2].set(coarser)
    return subband


def reference(quantized, scales):
    blocks = quantized.astype(jnp.float32).reshape(NZ, NY, NX // QB, QB)
    factor = jnp.transpose(scales, (1, 2, 0))[..., None]
    density = (blocks * factor).reshape(NZ, NY, NX)
    return decompose(density, 0).astype(jnp.bfloat16)
```

```python
import functools

import jax
import jax.numpy as jnp
import numpy as np
from jax import lax
from jax.experimental import pallas as pl
from jax.experimental.pallas import tpu as pltpu
from jax.sharding import PartitionSpec as P

LEVELS = 4
ALPHA = -1.586134342059924
BETA = -0.052980118572961
GAMMA = 0.882911075530934
DELTA = 0.443506852043971
KAPPA = 1.230174104914001

NZ, BY, BX = 16, 48, 128
OFF = (0, 16, 24, 28)
NP = 30
SR = (0, 0, 1, 3)
SL = (0, 1, 2, 0)
MESH = pl.DeviceIdType.MESH
F32, BF16 = jnp.float32, jnp.bfloat16


def lift_list(v):
    e, o = list(v[0::2]), list(v[1::2])
    m = len(e)
    up = lambda s: [s[min(i + 1, m - 1)] for i in range(m)]
    down = lambda s: [s[max(i - 1, 0)] for i in range(m)]
    o = [x + ALPHA * (a + b) for x, a, b in zip(o, e, up(e))]
    e = [x + BETA * (a + b) for x, a, b in zip(e, down(o), o)]
    o = [x + GAMMA * (a + b) for x, a, b in zip(o, e, up(e))]
    e = [x + DELTA * (a + b) for x, a, b in zip(e, down(o), o)]
    e = [x * (1.0 / KAPPA) for x in e]
    o = [x * (KAPPA / 2.0) for x in o]
    return [x for pair in zip(e, o) for x in pair]


def level_matrices(n):
    low, out = np.eye(n), []
    for _ in range(LEVELS):
        full = np.stack(lift_list(list(low)))
        out.append(full)
        low = full[::2]
    return out


def split(a):
    hi = a.astype(np.float32).astype(BF16)
    lo = (a - hi.astype(np.float64)).astype(np.float32).astype(BF16)
    return hi, lo


@functools.cache
def x_matrices():
    w = level_matrices(3 * BX)
    m = np.zeros((3, LEVELS, BX, 2 * BX))
    for v in range(3):
        for l in range(LEVELS):
            b, win = BX >> l, 8 << l
            mine = w[l][:, v * BX : (v + 1) * BX]
            for j in range(b):
                m[v, l, :, j << l] = mine[v * b + j]
            for start in range(0, BX, win):
                if v < 2:
                    for j in range(4 if l == 0 else 7):
                        lane = start + (j << l) + SR[l]
                        if j << l < win:
                            m[v, l, :, BX + lane] = mine[(v + 1) * b + j]
                if v > 0:
                    for j in range(1, 5 if l == 0 else 7):
                        lane = (start - (j << l) + SL[l]) % BX
                        m[v, l, :, BX + lane] = mine[v * b - j]
    hi, lo = split(m)
    return np.concatenate([hi, lo], axis=2)


@functools.cache
def y_matrices(groups):
    n = groups * BY
    w = level_matrices(n)
    m = np.zeros((groups, LEVELS, BY + 16, BY))
    for g in range(groups):
        for l in range(LEVELS):
            b = BY >> l
            mine = w[l][:, g * BY : (g + 1) * BY]
            for j in range(b):
                m[g, l, j << l] = mine[g * b + j]
            for k in range(8):
                r = (g + 1) * b + k
                if r < n >> l:
                    m[g, l, BY + k] = mine[r]
                r = g * b - 8 + k
                if r >= max((g - 1) * b, 0):
                    m[g, l, BY + 8 + k] = mine[r]
    hi, lo = split(m)
    return np.concatenate([hi, hi, lo], axis=3)


def hilo(x):
    hi = x.astype(BF16)
    return hi, (x - hi.astype(F32)).astype(BF16)


def stacked(x):
    hi, lo = hilo(x)
    return jnp.concatenate([hi, lo, hi], axis=0)


def dot(a, b):
    return jnp.dot(a, b, preferred_element_type=F32)


def lanes_of(shape):
    return lax.broadcasted_iota(jnp.int32, shape, len(shape) - 1)


def kernel(
    groups, tiles,
    q_hbm, s_hbm, mx_hbm, ay_hbm, out_ref,
    qv, sv, mxv, ayv, zh, zl, pk, from_left, from_right, yo,
    send0, send1, recv0, recv1, recv2,
    load_sem, xs_sem, xr_sem, ys_sem, yr_sem,
):
    g, t = lax.axis_index("grp"), lax.axis_index("tile")
    right, left = lax.rem(t + 1, tiles), lax.rem(t + tiles - 1, tiles)
    below, above = lax.rem(g + 1, groups), lax.rem(g + groups - 1, groups)
    below2, above2 = lax.rem(g + 2, groups), lax.rem(g + groups - 2, groups)

    barrier = pltpu.get_barrier_semaphore()
    for dev in ((g, left), (g, right), (above, t), (below, t), (above2, t), (below2, t)):
        pl.semaphore_signal(barrier, inc=1, device_id=dev, device_id_type=MESH)

    side = jnp.where(t == 0, 0, jnp.where(t == tiles - 1, 2, 1))
    loads = [
        pltpu.make_async_copy(q_hbm, qv, load_sem.at[0]),
        pltpu.make_async_copy(s_hbm, sv, load_sem.at[1]),
        pltpu.make_async_copy(mx_hbm.at[side], mxv, load_sem.at[2]),
        pltpu.make_async_copy(ay_hbm.at[g], ayv, load_sem.at[3]),
    ]
    for c in loads:
        c.start()
    loads[1].wait()
    loads[0].wait()

    st = jnp.transpose(sv[0])
    for c in range(3):
        rows = slice(16 * c, 16 * c + 16)
        band = [qv[z, rows, :].astype(F32) * st[rows, z : z + 1] for z in range(NZ)]
        for l in range(LEVELS):
            band = lift_list(band)
            for p, v in enumerate(band):
                hi, lo = hilo(v)
                zh[OFF[l] + p, rows, :] = hi
                zl[OFF[l] + p, rows, :] = lo
            band = band[0::2]

    loads[2].wait()
    own, packs = [], []
    lane = lanes_of((1, 1, BX))
    for l in range(LEVELS):
        n, win = NZ >> l, 8 << l
        h = zh[OFF[l] : OFF[l] + n].reshape(n * BY, BX)
        low = zl[OFF[l] : OFF[l] + n].reshape(n * BY, BX)
        mh, ml = mxv[l, :BX], mxv[l, BX:]
        r = dot(jnp.concatenate([h, low, h], axis=1), jnp.concatenate([mh, mh, ml], axis=0))
        own.append(r[:, :BX].reshape(n, BY, BX))
        if l == 0:
            plane = ((lane + 4) // 8) % NZ
        else:
            to_right = (lane % (1 << l)) == SR[l] % (1 << l)
            plane = jnp.where(to_right, lane // win, (lane // win + 1) % n)
        which = lax.broadcasted_iota(jnp.int32, (n, 1, BX), 0)
        packs.append(jnp.sum(jnp.where(which == plane, r[:, BX:].reshape(n, BY, BX), 0.0), axis=0))
    lane = lanes_of((BY, BX))
    pk[0] = jnp.where(lane % 2 == 0, packs[1], jnp.where(lane % 4 == 1, packs[2], packs[3]))
    pk[1] = packs[0]
    pk[2] = jnp.where(lane % 2 == 1, packs[1], jnp.where(lane % 4 == 2, packs[2], packs[3]))

    def remote(src, dst, ss, rs, dev):
        return pltpu.make_async_remote_copy(
            src_ref=src, dst_ref=dst, send_sem=ss, recv_sem=rs, device_id=dev, device_id_type=MESH
        )

    pl.semaphore_wait(barrier, 6)
    xcopies = [
        remote(pk.at[0:2], from_left, xs_sem.at[0], xr_sem.at[0], (g, right)),
        remote(pk.at[1:3], from_right, xs_sem.at[1], xr_sem.at[1], (g, left)),
    ]
    for c in xcopies:
        c.start()

    loads[3].wait()
    for l in range(LEVELS):
        n = NZ >> l
        r = dot(ayv[l], stacked(jnp.concatenate([own[l][p] for p in range(n)], axis=1)))
        for p in range(n):
            yo[OFF[l] + p] = r[:, p * BX : (p + 1) * BX]

    for c in xcopies:
        c.wait()
    edge0 = dot(
        ayv[0], stacked(jnp.where(lane % 8 < 4, from_left[1], from_right[0]))
    )
    edges = dot(
        ayv[1:].reshape(3 * (BY + 16), 3 * BY),
        stacked(jnp.concatenate([from_left[0], from_right[1]], axis=1)),
    )

    def edge_of(l, p, rows):
        n = rows.stop - rows.start
        lane = lanes_of((n, BX))
        win = 8 << l
        turned = lambda e, s: pltpu.roll(e, (-s) % BX, 1)
        if l == 0:
            return jnp.where((lane + 4) % BX < 8, turned(edge0[rows], 8 * p), 0.0)
        base = (l - 1) * (BY + 16)
        e = edges[base + rows.start : base + rows.stop]
        a = turned(e[:, :BX], win * p + SR[l])
        b = turned(e[:, BX:], win * p + SL[l])
        return jnp.where(lane < win, a, 0.0) + jnp.where(lane >= BX - win, b, 0.0)

    tail = slice(BY, BY + 16)
    for l in range(LEVELS):
        for p in range(NZ >> l):
            r = yo[OFF[l] + p, BY:, :] + edge_of(l, p, tail)
            if l == 0:
                send0[0, p] = r[0:4]
                send0[1, p] = r[12:16]
            else:
                send1[0, OFF[l] - NZ + p] = r[0:8]
                send1[1, OFF[l] - NZ + p] = r[8:16]
    ycopies = [
        remote(send0.at[0], recv0.at[0], ys_sem.at[0], yr_sem.at[0], (below, t)),
        remote(send0.at[1], recv0.at[1], ys_sem.at[1], yr_sem.at[1], (above, t)),
        remote(send1.at[0], recv1.at[0], ys_sem.at[2], yr_sem.at[2], (below, t)),
        remote(send1.at[1], recv1.at[1], ys_sem.at[3], yr_sem.at[3], (above, t)),
        remote(send1.at[0, 12:14], recv2, ys_sem.at[4], yr_sem.at[4], (below2, t)),
    ]
    for c in ycopies:
        c.start()

    row = lax.broadcasted_iota(jnp.int32, (BY, BX), 0)
    here = slice(0, BY)
    for z in range(NZ):
        value = None
        for l in reversed(range(LEVELS)):
            if z % (1 << l):
                continue
            p = z >> l
            part = yo[OFF[l] + p, :BY, :] + edge_of(l, p, here)
            if value is None:
                value = part
            else:
                step = 2 << l
                value = jnp.where((row % step == 0) & (lane % step == 0), value, part)
        yo[z, :BY, :] = value

    for c in ycopies:
        c.wait()
    lane = lanes_of((1, BX))

    def valid(l, p, j, v):
        if l and p % 2 == 0 and j % 2 == 0 and l < LEVELS - 1:
            return jnp.where(lane % (2 << l) == 1 << l, v, 0.0)
        if l:
            return jnp.where(lane % (1 << l) == 0, v, 0.0)
        if p % 2 == 0 and j % 2 == 0:
            return jnp.where(lane % 2 == 1, v, 0.0)
        return v

    for z in range(NZ):
        adds = {}
        for l in range(LEVELS):
            if z % (1 << l):
                continue
            p = z >> l
            for k in range(3 if l == 0 else 7):
                if k << l < BY:
                    v = recv0[0, p, k : k + 1, :] if l == 0 else recv1[0, OFF[l] - NZ + p, k : k + 1, :]
                    adds.setdefault(k << l, []).append(valid(l, p, k, v))
            for k in range(4 if l == 0 else 2, 8):
                r = BY - ((8 - k) << l)
                v = recv0[1, p, k - 4 : k - 3, :] if l == 0 else recv1[1, OFF[l] - NZ + p, k : k + 1, :]
                adds.setdefault(r, []).append(valid(l, p, k, v))
            if l == 3:
                adds[0].append(valid(l, p, 6, recv2[p, 6:7, :]))
        for r, vs in adds.items():
            yo[z, r : r + 1, :] = functools.reduce(lambda a, b: a + b, vs, yo[z, r : r + 1, :])
        out_ref[z] = yo[z, :BY, :].astype(BF16)


def body(quantized, scales):
    groups, tiles = lax.axis_size("grp"), lax.axis_size("tile")
    hbm = pl.BlockSpec(memory_space=pl.ANY)
    dma = pltpu.SemaphoreType.DMA
    return pl.pallas_call(
        functools.partial(kernel, groups, tiles),
        out_shape=jax.ShapeDtypeStruct((NZ, BY, BX), BF16),
        in_specs=[hbm] * 4,
        out_specs=pl.BlockSpec(memory_space=pltpu.VMEM),
        scratch_shapes=[
            pltpu.VMEM((NZ, BY, BX), BF16),
            pltpu.VMEM((1, NZ, BY), F32),
            pltpu.VMEM((LEVELS, 2 * BX, 2 * BX), BF16),
            pltpu.VMEM((LEVELS, BY + 16, 3 * BY), BF16),
            pltpu.VMEM((NP, BY, BX), BF16),
            pltpu.VMEM((NP, BY, BX), BF16),
            pltpu.VMEM((3, BY, BX), F32),
            pltpu.VMEM((2, BY, BX), F32),
            pltpu.VMEM((2, BY, BX), F32),
            pltpu.VMEM((NP, BY + 16, BX), F32),
            pltpu.VMEM((2, NZ, 4, BX), F32),
            pltpu.VMEM((2, NP - NZ, 8, BX), F32),
            pltpu.VMEM((2, NZ, 4, BX), F32),
            pltpu.VMEM((2, NP - NZ, 8, BX), F32),
            pltpu.VMEM((2, 8, BX), F32),
            dma((4,)), dma((2,)), dma((2,)), dma((5,)), dma((5,)),
        ],
        compiler_params=pltpu.CompilerParams(collective_id=0, has_side_effects=True),
    )(quantized, scales, jnp.asarray(x_matrices()), jnp.asarray(y_matrices(groups)))


def solution(mesh):
    return jax.shard_map(
        body,
        mesh=mesh,
        in_specs=(P(None, "grp", "tile"), P("tile", None, "grp")),
        out_specs=P(None, "grp", "tile"),
        check_vma=False,
    )
```

```python
import functools

import jax
import jax.numpy as jnp
import numpy as np
from jax import lax
from jax.experimental import pallas as pl
from jax.experimental.pallas import tpu as pltpu
from jax.sharding import PartitionSpec as P

LEVELS = 4
ALPHA = -1.586134342059924
BETA = -0.052980118572961
GAMMA = 0.882911075530934
DELTA = 0.443506852043971
KAPPA = 1.230174104914001

NZ, BY, BX = 16, 48, 128
OFF = (0, 16, 24, 28)
NP = 30
SR = (0, 0, 1, 3)
SL = (0, 1, 2, 0)
MESH = pl.DeviceIdType.MESH
F32, BF16 = jnp.float32, jnp.bfloat16


def lift_list(v):
    e, o = list(v[0::2]), list(v[1::2])
    m = len(e)
    up = lambda s: [s[min(i + 1, m - 1)] for i in range(m)]
    down = lambda s: [s[max(i - 1, 0)] for i in range(m)]
    o = [x + ALPHA * (a + b) for x, a, b in zip(o, e, up(e))]
    e = [x + BETA * (a + b) for x, a, b in zip(e, down(o), o)]
    o = [x + GAMMA * (a + b) for x, a, b in zip(o, e, up(e))]
    e = [x + DELTA * (a + b) for x, a, b in zip(e, down(o), o)]
    e = [x * (1.0 / KAPPA) for x in e]
    o = [x * (KAPPA / 2.0) for x in o]
    return [x for pair in zip(e, o) for x in pair]


def level_matrices(n):
    low, out = np.eye(n), []
    for _ in range(LEVELS):
        full = np.stack(lift_list(list(low)))
        out.append(full)
        low = full[::2]
    return out


def split(a):
    hi = a.astype(np.float32).astype(BF16)
    lo = (a - hi.astype(np.float64)).astype(np.float32).astype(BF16)
    return hi, lo


@functools.cache
def x_matrices():
    w = level_matrices(3 * BX)
    m = np.zeros((3, LEVELS, BX, 2 * BX))
    for v in range(3):
        for l in range(LEVELS):
            b, win = BX >> l, 8 << l
            mine = w[l][:, v * BX : (v + 1) * BX]
            for j in range(b):
                m[v, l, :, j << l] = mine[v * b + j]
            for start in range(0, BX, win):
                if v < 2:
                    for j in range(4 if l == 0 else 7):
                        lane = start + (j << l) + SR[l]
                        if j << l < win:
                            m[v, l, :, BX + lane] = mine[(v + 1) * b + j]
                if v > 0:
                    for j in range(1, 5 if l == 0 else 7):
                        lane = (start - (j << l) + SL[l]) % BX
                        m[v, l, :, BX + lane] = mine[v * b - j]
    hi, lo = split(m)
    return np.concatenate([hi, lo], axis=2)


@functools.cache
def y_matrices(groups):
    n = groups * BY
    w = level_matrices(n)
    m = np.zeros((groups, LEVELS, BY + 16, BY))
    for g in range(groups):
        for l in range(LEVELS):
            b = BY >> l
            mine = w[l][:, g * BY : (g + 1) * BY]
            for j in range(b):
                m[g, l, j << l] = mine[g * b + j]
            for k in range(8):
                r = (g + 1) * b + k
                if r < n >> l:
                    m[g, l, BY + k] = mine[r]
                r = g * b - 8 + k
                if r >= max((g - 1) * b, 0):
                    m[g, l, BY + 8 + k] = mine[r]
    hi, lo = split(m)
    return np.concatenate([hi, hi, lo], axis=3)


def hilo(x):
    hi = x.astype(BF16)
    return hi, (x - hi.astype(F32)).astype(BF16)


def stacked(x):
    hi, lo = hilo(x)
    return jnp.concatenate([hi, lo, hi], axis=0)


def dot(a, b):
    return jnp.dot(a, b, preferred_element_type=F32)


def lanes_of(shape):
    return lax.broadcasted_iota(jnp.int32, shape, len(shape) - 1)


def kernel(
    groups, tiles,
    q_hbm, s_hbm, mx_hbm, ay_hbm, out_ref,
    qv, sv, mxv, ayv, zh, zl, pk, from_left, from_right, yo,
    send0, send1, recv0, recv1, recv2,
    load_sem, xs_sem, xr_sem, ys_sem, yr_sem,
):
    g, t = lax.axis_index("grp"), lax.axis_index("tile")
    right, left = lax.rem(t + 1, tiles), lax.rem(t + tiles - 1, tiles)
    below, above = lax.rem(g + 1, groups), lax.rem(g + groups - 1, groups)
    below2, above2 = lax.rem(g + 2, groups), lax.rem(g + groups - 2, groups)

    has_left, has_right = t > 0, t < tiles - 1
    has_above, has_below = g > 0, g < groups - 1
    has_above2, has_below2 = g > 1, g < groups - 2
    barrier = pltpu.get_barrier_semaphore()
    for there, dev in (
        (has_left, (g, left)), (has_right, (g, right)),
        (has_above, (above, t)), (has_below, (below, t)),
        (has_above2, (above2, t)), (has_below2, (below2, t)),
    ):
        @pl.when(there)
        def _():
            pl.semaphore_signal(barrier, inc=1, device_id=dev, device_id_type=MESH)

    side = jnp.where(t == 0, 0, jnp.where(t == tiles - 1, 2, 1))
    loads = [
        pltpu.make_async_copy(q_hbm, qv, load_sem.at[0]),
        pltpu.make_async_copy(s_hbm, sv, load_sem.at[1]),
        pltpu.make_async_copy(mx_hbm.at[side], mxv, load_sem.at[2]),
        pltpu.make_async_copy(ay_hbm.at[g], ayv, load_sem.at[3]),
    ]
    for c in loads:
        c.start()
    for there, buffers in (
        (has_left, (from_left,)), (has_right, (from_right,)),
        (has_above, (recv0.at[0], recv1.at[0])), (has_below, (recv0.at[1], recv1.at[1])),
        (has_above2, (recv2,)),
    ):
        @pl.when(jnp.logical_not(there))
        def _():
            for b in buffers:
                b[...] = jnp.zeros(b.shape, F32)
    loads[1].wait()
    loads[0].wait()

    st = jnp.transpose(sv[0])
    for c in range(3):
        rows = slice(16 * c, 16 * c + 16)
        band = [qv[z, rows, :].astype(F32) * st[rows, z : z + 1] for z in range(NZ)]
        for l in range(LEVELS):
            band = lift_list(band)
            for p, v in enumerate(band):
                hi, lo = hilo(v)
                zh[OFF[l] + p, rows, :] = hi
                zl[OFF[l] + p, rows, :] = lo
            band = band[0::2]

    loads[2].wait()
    own, packs = [], []
    lane = lanes_of((1, 1, BX))
    for l in range(LEVELS):
        n, win = NZ >> l, 8 << l
        h = zh[OFF[l] : OFF[l] + n].reshape(n * BY, BX)
        low = zl[OFF[l] : OFF[l] + n].reshape(n * BY, BX)
        mh, ml = mxv[l, :BX], mxv[l, BX:]
        r = dot(jnp.concatenate([h, low, h], axis=1), jnp.concatenate([mh, mh, ml], axis=0))
        own.append(r[:, :BX].reshape(n, BY, BX))
        if l == 0:
            plane = ((lane + 4) // 8) % NZ
        else:
            to_right = (lane % (1 << l)) == SR[l] % (1 << l)
            plane = jnp.where(to_right, lane // win, (lane // win + 1) % n)
        which = lax.broadcasted_iota(jnp.int32, (n, 1, BX), 0)
        packs.append(jnp.sum(jnp.where(which == plane, r[:, BX:].reshape(n, BY, BX), 0.0), axis=0))
    lane = lanes_of((BY, BX))
    pk[0] = jnp.where(lane % 2 == 0, packs[1], jnp.where(lane % 4 == 1, packs[2], packs[3]))
    pk[1] = packs[0]
    pk[2] = jnp.where(lane % 2 == 1, packs[1], jnp.where(lane % 4 == 2, packs[2], packs[3]))

    def remote(src, dst, ss, rs, dev):
        return pltpu.make_async_remote_copy(
            src_ref=src, dst_ref=dst, send_sem=ss, recv_sem=rs, device_id=dev, device_id_type=MESH
        )

    def start(copies):
        for to, _, c in copies:
            pl.when(to)(c.start)

    def finish(copies):
        for to, came, c in copies:
            pl.when(came)(c.wait_recv)
        for to, came, c in copies:
            pl.when(to)(c.wait_send)

    neighbours = (
        jnp.where(has_left, 1, 0) + jnp.where(has_right, 1, 0) + jnp.where(has_above, 1, 0)
        + jnp.where(has_below, 1, 0) + jnp.where(has_above2, 1, 0) + jnp.where(has_below2, 1, 0)
    )
    pl.semaphore_wait(barrier, neighbours)
    xcopies = [
        (has_right, has_left, remote(pk.at[0:2], from_left, xs_sem.at[0], xr_sem.at[0], (g, right))),
        (has_left, has_right, remote(pk.at[1:3], from_right, xs_sem.at[1], xr_sem.at[1], (g, left))),
    ]
    start(xcopies)

    loads[3].wait()
    for l in range(LEVELS):
        n = NZ >> l
        r = dot(ayv[l], stacked(jnp.concatenate([own[l][p] for p in range(n)], axis=1)))
        for p in range(n):
            yo[OFF[l] + p] = r[:, p * BX : (p + 1) * BX]

    finish(xcopies)
    edge0 = dot(
        ayv[0], stacked(jnp.where(lane % 8 < 4, from_left[1], from_right[0]))
    )
    edges = dot(
        ayv[1:].reshape(3 * (BY + 16), 3 * BY),
        stacked(jnp.concatenate([from_left[0], from_right[1]], axis=1)),
    )

    def edge_of(l, p, rows):
        n = rows.stop - rows.start
        lane = lanes_of((n, BX))
        win = 8 << l
        turned = lambda e, s: pltpu.roll(e, (-s) % BX, 1)
        if l == 0:
            return jnp.where((lane + 4) % BX < 8, turned(edge0[rows], 8 * p), 0.0)
        base = (l - 1) * (BY + 16)
        e = edges[base + rows.start : base + rows.stop]
        a = turned(e[:, :BX], win * p + SR[l])
        b = turned(e[:, BX:], win * p + SL[l])
        return jnp.where(lane < win, a, 0.0) + jnp.where(lane >= BX - win, b, 0.0)

    tail = slice(BY, BY + 16)
    for l in range(LEVELS):
        for p in range(NZ >> l):
            r = yo[OFF[l] + p, BY:, :] + edge_of(l, p, tail)
            if l == 0:
                send0[0, p] = r[0:4]
                send0[1, p] = r[12:16]
            else:
                send1[0, OFF[l] - NZ + p] = r[0:8]
                send1[1, OFF[l] - NZ + p] = r[8:16]
    ycopies = [
        (has_below, has_above, remote(send0.at[0], recv0.at[0], ys_sem.at[0], yr_sem.at[0], (below, t))),
        (has_above, has_below, remote(send0.at[1], recv0.at[1], ys_sem.at[1], yr_sem.at[1], (above, t))),
        (has_below, has_above, remote(send1.at[0], recv1.at[0], ys_sem.at[2], yr_sem.at[2], (below, t))),
        (has_above, has_below, remote(send1.at[1], recv1.at[1], ys_sem.at[3], yr_sem.at[3], (above, t))),
        (has_below2, has_above2, remote(send1.at[0, 12:14], recv2, ys_sem.at[4], yr_sem.at[4], (below2, t))),
    ]
    start(ycopies)

    row = lax.broadcasted_iota(jnp.int32, (BY, BX), 0)
    here = slice(0, BY)
    for z in range(NZ):
        value = None
        for l in reversed(range(LEVELS)):
            if z % (1 << l):
                continue
            p = z >> l
            part = yo[OFF[l] + p, :BY, :] + edge_of(l, p, here)
            if value is None:
                value = part
            else:
                step = 2 << l
                value = jnp.where((row % step == 0) & (lane % step == 0), value, part)
        yo[z, :BY, :] = value

    finish(ycopies)
    lane = lanes_of((1, BX))

    def valid(l, p, j, v):
        if l and p % 2 == 0 and j % 2 == 0 and l < LEVELS - 1:
            return jnp.where(lane % (2 << l) == 1 << l, v, 0.0)
        if l:
            return jnp.where(lane % (1 << l) == 0, v, 0.0)
        if p % 2 == 0 and j % 2 == 0:
            return jnp.where(lane % 2 == 1, v, 0.0)
        return v

    for z in range(NZ):
        adds = {}
        for l in range(LEVELS):
            if z % (1 << l):
                continue
            p = z >> l
            for k in range(3 if l == 0 else 7):
                if k << l < BY:
                    v = recv0[0, p, k : k + 1, :] if l == 0 else recv1[0, OFF[l] - NZ + p, k : k + 1, :]
                    adds.setdefault(k << l, []).append(valid(l, p, k, v))
            for k in range(4 if l == 0 else 2, 8):
                r = BY - ((8 - k) << l)
                v = recv0[1, p, k - 4 : k - 3, :] if l == 0 else recv1[1, OFF[l] - NZ + p, k : k + 1, :]
                adds.setdefault(r, []).append(valid(l, p, k, v))
            if l == 3:
                adds[0].append(valid(l, p, 6, recv2[p, 6:7, :]))
        for r, vs in adds.items():
            yo[z, r : r + 1, :] = functools.reduce(lambda a, b: a + b, vs, yo[z, r : r + 1, :])
        out_ref[z] = yo[z, :BY, :].astype(BF16)


def body(quantized, scales):
    groups, tiles = lax.axis_size("grp"), lax.axis_size("tile")
    hbm = pl.BlockSpec(memory_space=pl.ANY)
    dma = pltpu.SemaphoreType.DMA
    return pl.pallas_call(
        functools.partial(kernel, groups, tiles),
        out_shape=jax.ShapeDtypeStruct((NZ, BY, BX), BF16),
        in_specs=[hbm] * 4,
        out_specs=pl.BlockSpec(memory_space=pltpu.VMEM),
        scratch_shapes=[
            pltpu.VMEM((NZ, BY, BX), BF16),
            pltpu.VMEM((1, NZ, BY), F32),
            pltpu.VMEM((LEVELS, 2 * BX, 2 * BX), BF16),
            pltpu.VMEM((LEVELS, BY + 16, 3 * BY), BF16),
            pltpu.VMEM((NP, BY, BX), BF16),
            pltpu.VMEM((NP, BY, BX), BF16),
            pltpu.VMEM((3, BY, BX), F32),
            pltpu.VMEM((2, BY, BX), F32),
            pltpu.VMEM((2, BY, BX), F32),
            pltpu.VMEM((NP, BY + 16, BX), F32),
            pltpu.VMEM((2, NZ, 4, BX), F32),
            pltpu.VMEM((2, NP - NZ, 8, BX), F32),
            pltpu.VMEM((2, NZ, 4, BX), F32),
            pltpu.VMEM((2, NP - NZ, 8, BX), F32),
            pltpu.VMEM((2, 8, BX), F32),
            dma((4,)), dma((2,)), dma((2,)), dma((5,)), dma((5,)),
        ],
        compiler_params=pltpu.CompilerParams(collective_id=0, has_side_effects=True),
    )(quantized, scales, jnp.asarray(x_matrices()), jnp.asarray(y_matrices(groups)))


def solution(mesh):
    return jax.shard_map(
        body,
        mesh=mesh,
        in_specs=(P(None, "grp", "tile"), P("tile", None, "grp")),
        out_specs=P(None, "grp", "tile"),
        check_vma=False,
    )
```

```python
import functools

import jax
import jax.numpy as jnp
import numpy as np
from jax import lax
from jax.experimental import pallas as pl
from jax.experimental.pallas import tpu as pltpu
from jax.sharding import PartitionSpec as P

LEVELS = 4
ALPHA = -1.586134342059924
BETA = -0.052980118572961
GAMMA = 0.882911075530934
DELTA = 0.443506852043971
KAPPA = 1.230174104914001

NZ, BY, BX = 16, 48, 128
OFF = (0, 16, 24, 28)
NP = 30
SR = (0, 0, 1, 3)
SL = (0, 1, 2, 0)
MESH = pl.DeviceIdType.MESH
F32, BF16 = jnp.float32, jnp.bfloat16


def lift_list(v):
    e, o = list(v[0::2]), list(v[1::2])
    m = len(e)
    up = lambda s: [s[min(i + 1, m - 1)] for i in range(m)]
    down = lambda s: [s[max(i - 1, 0)] for i in range(m)]
    o = [x + ALPHA * (a + b) for x, a, b in zip(o, e, up(e))]
    e = [x + BETA * (a + b) for x, a, b in zip(e, down(o), o)]
    o = [x + GAMMA * (a + b) for x, a, b in zip(o, e, up(e))]
    e = [x + DELTA * (a + b) for x, a, b in zip(e, down(o), o)]
    e = [x * (1.0 / KAPPA) for x in e]
    o = [x * (KAPPA / 2.0) for x in o]
    return [x for pair in zip(e, o) for x in pair]


def level_matrices(n):
    low, out = np.eye(n), []
    for _ in range(LEVELS):
        full = np.stack(lift_list(list(low)))
        out.append(full)
        low = full[::2]
    return out


def split(a):
    hi = a.astype(np.float32).astype(BF16)
    lo = (a - hi.astype(np.float64)).astype(np.float32).astype(BF16)
    return hi, lo


@functools.cache
def x_matrices():
    w = level_matrices(3 * BX)
    m = np.zeros((3, LEVELS, BX, 2 * BX))
    for v in range(3):
        for l in range(LEVELS):
            b, win = BX >> l, 8 << l
            mine = w[l][:, v * BX : (v + 1) * BX]
            for j in range(b):
                m[v, l, :, j << l] = mine[v * b + j]
            for start in range(0, BX, win):
                if v < 2:
                    for j in range(4 if l == 0 else 7):
                        lane = start + (j << l) + SR[l]
                        if j << l < win:
                            m[v, l, :, BX + lane] = mine[(v + 1) * b + j]
                if v > 0:
                    for j in range(1, 5 if l == 0 else 7):
                        lane = (start - (j << l) + SL[l]) % BX
                        m[v, l, :, BX + lane] = mine[v * b - j]
    hi, lo = split(m)
    return np.concatenate([hi, lo], axis=2)


@functools.cache
def y_matrices(groups):
    n = groups * BY
    w = level_matrices(n)
    m = np.zeros((groups, LEVELS, BY + 16, BY))
    for g in range(groups):
        for l in range(LEVELS):
            b = BY >> l
            mine = w[l][:, g * BY : (g + 1) * BY]
            for j in range(b):
                m[g, l, j << l] = mine[g * b + j]
            for k in range(8):
                r = (g + 1) * b + k
                if r < n >> l:
                    m[g, l, BY + k] = mine[r]
                r = g * b - 8 + k
                if r >= max((g - 1) * b, 0):
                    m[g, l, BY + 8 + k] = mine[r]
    hi, lo = split(m)
    return np.concatenate([hi, hi, lo], axis=3)


def hilo(x):
    hi = x.astype(BF16)
    return hi, (x - hi.astype(F32)).astype(BF16)


def stacked(x):
    hi, lo = hilo(x)
    return jnp.concatenate([hi, lo, hi], axis=0)


def dot(a, b):
    return jnp.dot(a, b, preferred_element_type=F32)


def lanes_of(shape):
    return lax.broadcasted_iota(jnp.int32, shape, len(shape) - 1)


def kernel(
    groups, tiles,
    q_hbm, s_hbm, mx_hbm, ay_hbm, out_ref,
    qv, sv, mxv, ayv, zh, zl, pk, from_left, from_right, yo,
    send0, send1, send2, recv0, recv1, recv2, recv3, recv4,
    load_sem, xs_sem, xr_sem, ys_sem, yr_sem,
):
    g, t = lax.axis_index("grp"), lax.axis_index("tile")
    right, left = lax.rem(t + 1, tiles), lax.rem(t + tiles - 1, tiles)
    below, above = lax.rem(g + 1, groups), lax.rem(g + groups - 1, groups)
    below2, above2 = lax.rem(g + 2, groups), lax.rem(g + groups - 2, groups)

    has_left, has_right = t > 0, t < tiles - 1
    has_above, has_below = g > 0, g < groups - 1
    has_above2, has_below2 = g > 1, g < groups - 2
    barrier = pltpu.get_barrier_semaphore()
    for there, dev in (
        (has_left, (g, left)), (has_right, (g, right)),
        (has_above, (above, t)), (has_below, (below, t)),
        (has_above2, (above2, t)), (has_below2, (below2, t)),
    ):
        @pl.when(there)
        def _():
            pl.semaphore_signal(barrier, inc=1, device_id=dev, device_id_type=MESH)

    side = jnp.where(t == 0, 0, jnp.where(t == tiles - 1, 2, 1))
    loads = [
        pltpu.make_async_copy(q_hbm, qv, load_sem.at[0]),
        pltpu.make_async_copy(s_hbm, sv, load_sem.at[1]),
        pltpu.make_async_copy(mx_hbm.at[side], mxv, load_sem.at[2]),
        pltpu.make_async_copy(ay_hbm.at[g], ayv, load_sem.at[3]),
    ]
    for c in loads:
        c.start()
    for there, buffers in (
        (has_left, (from_left,)), (has_right, (from_right,)),
        (has_above, (recv0.at[0], recv1.at[0], recv3.at[0])),
        (has_below, (recv0.at[1], recv1.at[1], recv3.at[1])),
        (has_above2, (recv2, recv4)),
    ):
        @pl.when(jnp.logical_not(there))
        def _():
            for b in buffers:
                b[...] = jnp.zeros(b.shape, F32)
    loads[1].wait()
    loads[0].wait()

    st = jnp.transpose(sv[0])
    for c in range(3):
        rows = slice(16 * c, 16 * c + 16)
        band = [qv[z, rows, :].astype(F32) * st[rows, z : z + 1] for z in range(NZ)]
        for l in range(LEVELS):
            band = lift_list(band)
            for p, v in enumerate(band):
                hi, lo = hilo(v)
                zh[OFF[l] + p, rows, :] = hi
                zl[OFF[l] + p, rows, :] = lo
            band = band[0::2]

    loads[2].wait()
    own, packs = [], []
    lane = lanes_of((1, 1, BX))
    for l in range(LEVELS):
        n, win = NZ >> l, 8 << l
        h = zh[OFF[l] : OFF[l] + n].reshape(n * BY, BX)
        low = zl[OFF[l] : OFF[l] + n].reshape(n * BY, BX)
        mh, ml = mxv[l, :BX], mxv[l, BX:]
        r = dot(jnp.concatenate([h, low, h], axis=1), jnp.concatenate([mh, mh, ml], axis=0))
        own.append(r[:, :BX].reshape(n, BY, BX))
        if l == 0:
            plane = ((lane + 4) // 8) % NZ
        else:
            to_right = (lane % (1 << l)) == SR[l] % (1 << l)
            plane = jnp.where(to_right, lane // win, (lane // win + 1) % n)
        which = lax.broadcasted_iota(jnp.int32, (n, 1, BX), 0)
        packs.append(jnp.sum(jnp.where(which == plane, r[:, BX:].reshape(n, BY, BX), 0.0), axis=0))
    lane = lanes_of((BY, BX))
    pk[0] = jnp.where(lane % 2 == 0, packs[1], jnp.where(lane % 4 == 1, packs[2], packs[3]))
    pk[1] = packs[0]
    pk[2] = jnp.where(lane % 2 == 1, packs[1], jnp.where(lane % 4 == 2, packs[2], packs[3]))

    def remote(src, dst, ss, rs, dev):
        return pltpu.make_async_remote_copy(
            src_ref=src, dst_ref=dst, send_sem=ss, recv_sem=rs, device_id=dev, device_id_type=MESH
        )

    def start(copies):
        for to, _, c in copies:
            pl.when(to)(c.start)

    def finish(copies):
        for to, came, c in copies:
            pl.when(came)(c.wait_recv)
        for to, came, c in copies:
            pl.when(to)(c.wait_send)

    neighbours = (
        jnp.where(has_left, 1, 0) + jnp.where(has_right, 1, 0) + jnp.where(has_above, 1, 0)
        + jnp.where(has_below, 1, 0) + jnp.where(has_above2, 1, 0) + jnp.where(has_below2, 1, 0)
    )
    pl.semaphore_wait(barrier, neighbours)
    xcopies = [
        (has_right, has_left, remote(pk.at[0:2], from_left, xs_sem.at[0], xr_sem.at[0], (g, right))),
        (has_left, has_right, remote(pk.at[1:3], from_right, xs_sem.at[1], xr_sem.at[1], (g, left))),
    ]
    start(xcopies)

    loads[3].wait()
    for l in range(LEVELS):
        n = NZ >> l
        r = dot(ayv[l], stacked(jnp.concatenate([own[l][p] for p in range(n)], axis=1)))
        for p in range(n):
            v = r[:, p * BX : (p + 1) * BX]
            yo[OFF[l] + p] = v[:BY]
            if l == 0:
                send0[0, p] = v[BY : BY + 4]
                send0[1, p] = v[BY + 12 :]
            else:
                send1[0, OFF[l] - NZ + p] = v[BY : BY + 8]
                send1[1, OFF[l] - NZ + p] = v[BY + 8 :]
    y1copies = [
        (has_below, has_above, remote(send0.at[0], recv0.at[0], ys_sem.at[0], yr_sem.at[0], (below, t))),
        (has_above, has_below, remote(send0.at[1], recv0.at[1], ys_sem.at[1], yr_sem.at[1], (above, t))),
        (has_below, has_above, remote(send1.at[0], recv1.at[0], ys_sem.at[2], yr_sem.at[2], (below, t))),
        (has_above, has_below, remote(send1.at[1], recv1.at[1], ys_sem.at[3], yr_sem.at[3], (above, t))),
        (has_below2, has_above2, remote(send1.at[0, 12:14], recv2, ys_sem.at[4], yr_sem.at[4], (below2, t))),
    ]
    start(y1copies)

    finish(xcopies)
    edge = stacked(
        jnp.concatenate(
            [jnp.where(lane % 8 < 4, from_left[1], from_right[0]), from_left[0], from_right[1]], axis=1
        )
    )
    r = dot(jnp.concatenate([ayv[l, BY:] for l in range(LEVELS)], axis=0), edge)
    far = [r[16 * l : 16 * l + 16] for l in range(LEVELS)]
    part = lambda l, k: far[l][:, k * BX : (k + 1) * BX]
    w = lanes_of((16, BX))
    for k, v in enumerate((
        part(0, 0),
        jnp.where(w % 2 == 0, part(1, 1), jnp.where(w % 4 == 1, part(2, 1), part(3, 1))),
        jnp.where(w % 2 == 1, part(1, 2), jnp.where(w % 4 == 2, part(2, 2), part(3, 2))),
    )):
        send2[0, k] = v[:8]
        send2[1, k] = v[8:]
    y2copies = [
        (has_below, has_above, remote(send2.at[0], recv3.at[0], ys_sem.at[5], yr_sem.at[5], (below, t))),
        (has_above, has_below, remote(send2.at[1], recv3.at[1], ys_sem.at[6], yr_sem.at[6], (above, t))),
        (has_below2, has_above2, remote(send2.at[0], recv4, ys_sem.at[7], yr_sem.at[7], (below2, t))),
    ]
    start(y2copies)

    def spread(l, p, packed0, packed_r, packed_l):
        win = 8 << l
        turned = lambda e, s: pltpu.roll(e, (-s) % BX, 1)
        if l == 0:
            return jnp.where((lanes_of(packed0.shape) + 4) % BX < 8, turned(packed0, 8 * p), 0.0)
        w = lanes_of(packed_r.shape)
        a = jnp.where(w < win, turned(packed_r, win * p + SR[l]), 0.0)
        return a + jnp.where(w >= BX - win, turned(packed_l, win * p + SL[l]), 0.0)

    r = dot(jnp.concatenate([ayv[l, :BY] for l in range(LEVELS)], axis=0), edge)
    near = [r[BY * l : BY * l + BY] for l in range(LEVELS)]

    row = lax.broadcasted_iota(jnp.int32, (BY, BX), 0)
    for z in range(NZ):
        value = None
        for l in reversed(range(LEVELS)):
            if z % (1 << l):
                continue
            p = z >> l
            part = yo[OFF[l] + p] + spread(l, p, *(near[l][:, k * BX : (k + 1) * BX] for k in range(3)))
            if value is None:
                value = part
            else:
                step = 2 << l
                value = jnp.where((row % step == 0) & (lane % step == 0), value, part)
        yo[z] = value

    finish(y1copies)
    finish(y2copies)
    lane = lanes_of((1, BX))
    outer = [jnp.concatenate([recv3[0, k], recv3[1, k]], axis=0) for k in range(3)]

    def valid(l, p, j, v):
        if l and p % 2 == 0 and j % 2 == 0 and l < LEVELS - 1:
            return jnp.where(lane % (2 << l) == 1 << l, v, 0.0)
        if l:
            return jnp.where(lane % (1 << l) == 0, v, 0.0)
        if p % 2 == 0 and j % 2 == 0:
            return jnp.where(lane % 2 == 1, v, 0.0)
        return v

    for z in range(NZ):
        adds = {}
        for l in range(LEVELS):
            if z % (1 << l):
                continue
            p = z >> l
            e = spread(l, p, *outer)
            if l == 0:
                down, up = recv0[0, p] + e[:4], recv0[1, p] + e[12:]
            else:
                down, up = recv1[0, OFF[l] - NZ + p] + e[:8], recv1[1, OFF[l] - NZ + p] + e[8:]
            for k in range(3 if l == 0 else 7):
                if k << l < BY:
                    adds.setdefault(k << l, []).append(valid(l, p, k, down[k : k + 1]))
            for k in range(4 if l == 0 else 2, 8):
                adds.setdefault(BY - ((8 - k) << l), []).append(valid(l, p, k, up[k - 4 : k - 3] if l == 0 else up[k : k + 1]))
            if l == 3:
                v = recv2[p] + spread(l, p, None, recv4[1], recv4[2])
                adds[0].append(valid(l, p, 6, v[6:7]))
        for r, vs in adds.items():
            yo[z, r : r + 1, :] = functools.reduce(lambda a, b: a + b, vs, yo[z, r : r + 1, :])
        out_ref[z] = yo[z].astype(BF16)


def body(quantized, scales):
    groups, tiles = lax.axis_size("grp"), lax.axis_size("tile")
    hbm = pl.BlockSpec(memory_space=pl.ANY)
    dma = pltpu.SemaphoreType.DMA
    return pl.pallas_call(
        functools.partial(kernel, groups, tiles),
        out_shape=pltpu.VMEM((NZ, BY, BX), BF16),
        in_specs=[hbm] * 4,

        scratch_shapes=[
            pltpu.VMEM((NZ, BY, BX), BF16),
            pltpu.VMEM((1, NZ, BY), F32),
            pltpu.VMEM((LEVELS, 2 * BX, 2 * BX), BF16),
            pltpu.VMEM((LEVELS, BY + 16, 3 * BY), BF16),
            pltpu.VMEM((NP, BY, BX), BF16),
            pltpu.VMEM((NP, BY, BX), BF16),
            pltpu.VMEM((3, BY, BX), F32),
            pltpu.VMEM((2, BY, BX), F32),
            pltpu.VMEM((2, BY, BX), F32),
            pltpu.VMEM((NP, BY, BX), F32),
            pltpu.VMEM((2, NZ, 4, BX), F32),
            pltpu.VMEM((2, NP - NZ, 8, BX), F32),
            pltpu.VMEM((2, 3, 8, BX), F32),
            pltpu.VMEM((2, NZ, 4, BX), F32),
            pltpu.VMEM((2, NP - NZ, 8, BX), F32),
            pltpu.VMEM((2, 8, BX), F32),
            pltpu.VMEM((2, 3, 8, BX), F32),
            pltpu.VMEM((3, 8, BX), F32),
            dma((4,)), dma((2,)), dma((2,)), dma((8,)), dma((8,)),
        ],
        compiler_params=pltpu.CompilerParams(collective_id=0, has_side_effects=True),
    )(quantized, scales, jnp.asarray(x_matrices()), jnp.asarray(y_matrices(groups)))


def solution(mesh):
    return jax.shard_map(
        body,
        mesh=mesh,
        in_specs=(P(None, "grp", "tile"), P("tile", None, "grp")),
        out_specs=P(None, "grp", "tile"),
        check_vma=False,
    )
```

```python
import functools

import jax
import jax.numpy as jnp
import numpy as np
from jax import lax
from jax.experimental import pallas as pl
from jax.experimental.pallas import tpu as pltpu
from jax.sharding import PartitionSpec as P

LEVELS = 4
ALPHA = -1.586134342059924
BETA = -0.052980118572961
GAMMA = 0.882911075530934
DELTA = 0.443506852043971
KAPPA = 1.230174104914001

NZ, BY, BX = 16, 48, 128
OFF = (0, 16, 24, 28)
NP = 30
SR = (0, 0, 1, 3)
SL = (0, 1, 2, 0)
SLOT = (0, 0, 4, 5)
MESH = pl.DeviceIdType.MESH
F32, BF16 = jnp.float32, jnp.bfloat16


def lift_list(v):
    e, o = list(v[0::2]), list(v[1::2])
    m = len(e)
    up = lambda s: [s[min(i + 1, m - 1)] for i in range(m)]
    down = lambda s: [s[max(i - 1, 0)] for i in range(m)]
    o = [x + ALPHA * (a + b) for x, a, b in zip(o, e, up(e))]
    e = [x + BETA * (a + b) for x, a, b in zip(e, down(o), o)]
    o = [x + GAMMA * (a + b) for x, a, b in zip(o, e, up(e))]
    e = [x + DELTA * (a + b) for x, a, b in zip(e, down(o), o)]
    e = [x * (1.0 / KAPPA) for x in e]
    o = [x * (KAPPA / 2.0) for x in o]
    return [x for pair in zip(e, o) for x in pair]


def level_matrices(n):
    low, out = np.eye(n), []
    for _ in range(LEVELS):
        full = np.stack(lift_list(list(low)))
        out.append(full)
        low = full[::2]
    return out


def split(a):
    hi = a.astype(np.float32).astype(BF16)
    lo = (a - hi.astype(np.float64)).astype(np.float32).astype(BF16)
    return hi, lo


def hi_hi_lo(a):
    hi, lo = split(a)
    return np.concatenate([hi, hi, lo], axis=-1)


@functools.cache
def x_matrices():
    w = level_matrices(3 * BX)
    m = np.zeros((3, LEVELS, BX, 2 * BX))
    for v in range(3):
        for l in range(LEVELS):
            b, win = BX >> l, 8 << l
            mine = w[l][:, v * BX : (v + 1) * BX]
            for j in range(b):
                m[v, l, :, j << l] = mine[v * b + j]
            for start in range(0, BX, win):
                if v < 2:
                    for j in range(4 if l == 0 else 7):
                        lane = start + (j << l) + SR[l]
                        if j << l < win:
                            m[v, l, :, BX + lane] = mine[(v + 1) * b + j]
                if v > 0:
                    for j in range(1, 5 if l == 0 else 7):
                        lane = (start - (j << l) + SL[l]) % BX
                        m[v, l, :, BX + lane] = mine[v * b - j]
    hi, lo = split(m)
    return np.concatenate([hi, lo], axis=2)


@functools.cache
def y_matrices(groups):
    n = groups * BY
    w = level_matrices(n)
    m = np.zeros((groups, LEVELS, BY + 16, BY))
    for g in range(groups):
        for l in range(LEVELS):
            b = BY >> l
            mine = w[l][:, g * BY : (g + 1) * BY]
            for j in range(b):
                m[g, l, j << l] = mine[g * b + j]
            for k in range(8):
                r = (g + 1) * b + k
                if r < n >> l:
                    m[g, l, BY + k] = mine[r]
                r = g * b - 8 + k
                if r >= max((g - 1) * b, 0):
                    m[g, l, BY + 8 + k] = mine[r]
    return hi_hi_lo(m)


@functools.cache
def packed_matrices(groups):
    m = y_matrices(groups)
    out = np.zeros((groups, LEVELS - 1, 40, 3 * BY), m.dtype)
    for l in range(1, LEVELS):
        out[:, l - 1, : BY >> l] = m[:, l, : BY : 1 << l]
        out[:, l - 1, 24:] = m[:, l, BY:]
    return out


def hilo(x):
    hi = x.astype(BF16)
    return hi, (x - hi.astype(F32)).astype(BF16)


def stacked(x):
    hi, lo = hilo(x)
    return jnp.concatenate([hi, lo, hi], axis=0)


def dot(a, b):
    return jnp.dot(a, b, preferred_element_type=F32)


def lanes_of(shape):
    return lax.broadcasted_iota(jnp.int32, shape, len(shape) - 1)


def kernel(
    groups, tiles,
    q_hbm, s_hbm, mx_hbm, ay_hbm, ac_hbm, out_ref,
    qv, sv, mxv, ayv, acv, zh, zl, to_right, to_left, from_left, from_right, wide, yo,
    send0, send1, send2, recv0, recv1, recv2, recv3, recv4,
    load_sem, xs_sem, xr_sem, ys_sem, yr_sem,
):
    g, t = lax.axis_index("grp"), lax.axis_index("tile")
    right, left = lax.rem(t + 1, tiles), lax.rem(t + tiles - 1, tiles)
    below, above = lax.rem(g + 1, groups), lax.rem(g + groups - 1, groups)
    below2, above2 = lax.rem(g + 2, groups), lax.rem(g + groups - 2, groups)

    has_left, has_right = t > 0, t < tiles - 1
    has_above, has_below = g > 0, g < groups - 1
    has_above2, has_below2 = g > 1, g < groups - 2
    barrier = pltpu.get_barrier_semaphore()
    for there, dev in (
        (has_left, (g, left)), (has_right, (g, right)),
        (has_above, (above, t)), (has_below, (below, t)),
        (has_above2, (above2, t)), (has_below2, (below2, t)),
    ):
        @pl.when(there)
        def _():
            pl.semaphore_signal(barrier, inc=1, device_id=dev, device_id_type=MESH)

    side = jnp.where(t == 0, 0, jnp.where(t == tiles - 1, 2, 1))
    loads = [
        pltpu.make_async_copy(q_hbm, qv, load_sem.at[0]),
        pltpu.make_async_copy(s_hbm, sv, load_sem.at[1]),
        pltpu.make_async_copy(mx_hbm.at[side], mxv, load_sem.at[2]),
        pltpu.make_async_copy(ay_hbm.at[g], ayv, load_sem.at[3]),
        pltpu.make_async_copy(ac_hbm.at[g], acv, load_sem.at[4]),
    ]
    for c in loads:
        c.start()
    for there, buffers in (
        (has_left, (from_left,)), (has_right, (from_right,)),
        (has_above, (recv0.at[0], recv1.at[0], recv3.at[0])),
        (has_below, (recv0.at[1], recv1.at[1], recv3.at[1])),
        (has_above2, (recv2, recv4)),
    ):
        @pl.when(jnp.logical_not(there))
        def _():
            for b in buffers:
                b[...] = jnp.zeros(b.shape, F32)
    loads[1].wait()
    loads[0].wait()

    st = jnp.transpose(sv[0])
    for c in range(3):
        rows = slice(16 * c, 16 * c + 16)
        band = [qv[z, rows, :].astype(F32) * st[rows, z : z + 1] for z in range(NZ)]
        for l in range(LEVELS):
            band = lift_list(band)
            for p, v in enumerate(band):
                hi, lo = hilo(v)
                zh[OFF[l] + p, rows, :] = hi
                zl[OFF[l] + p, rows, :] = lo
            band = band[0::2]

    loads[2].wait()
    own, packs = [], []
    lane = lanes_of((1, 1, BX))
    for l in range(LEVELS):
        n, win = NZ >> l, 8 << l
        h = zh[OFF[l] : OFF[l] + n].reshape(n * BY, BX)
        low = zl[OFF[l] : OFF[l] + n].reshape(n * BY, BX)
        mh, ml = mxv[l, :BX], mxv[l, BX:]
        r = dot(jnp.concatenate([h, low, h], axis=1), jnp.concatenate([mh, mh, ml], axis=0))
        own.append(r[:, :BX].reshape(n, BY, BX))
        if l == 0:
            plane = ((lane + 4) // 8) % NZ
        else:
            rightward = (lane % (1 << l)) == SR[l] % (1 << l)
            plane = jnp.where(rightward, lane // win, (lane // win + 1) % n)
        which = lax.broadcasted_iota(jnp.int32, (n, 1, BX), 0)
        packs.append(jnp.sum(jnp.where(which == plane, r[:, BX:].reshape(n, BY, BX), 0.0), axis=0))

    loads[3].wait()
    loads[4].wait()
    e0 = dot(ayv[0], stacked(packs[0]))
    e1, e2, e3 = (dot(acv[l - 1], stacked(packs[l])) for l in range(1, LEVELS))
    lane = lanes_of((24, BX))
    to_right[:24] = jnp.where(lane % 8 < 4, e0[:24], pltpu.roll(e0[24:48], 4, 1))
    to_left[:24] = jnp.where(lane % 8 >= 4, e0[:24], pltpu.roll(e0[24:48], BX - 4, 1))
    to_right[24:32] = e0[48:56] + e0[56:]
    to_left[24:32] = e0[48:56] + e0[56:]
    lane = lanes_of((40, BX))
    to_right[32:] = jnp.where(lane % 2 == 0, e1, jnp.where(lane % 4 == 1, e2, e3))
    to_left[32:] = jnp.where(lane % 2 == 1, e1, jnp.where(lane % 4 == 2, e2, e3))
    lane = lanes_of((BY, BX))

    def remote(src, dst, ss, rs, dev):
        return pltpu.make_async_remote_copy(
            src_ref=src, dst_ref=dst, send_sem=ss, recv_sem=rs, device_id=dev, device_id_type=MESH
        )

    def start(copies):
        for to, _, c in copies:
            pl.when(to)(c.start)

    def finish(copies):
        for to, came, c in copies:
            pl.when(came)(c.wait_recv)
        for to, came, c in copies:
            pl.when(to)(c.wait_send)

    neighbours = (
        jnp.where(has_left, 1, 0) + jnp.where(has_right, 1, 0) + jnp.where(has_above, 1, 0)
        + jnp.where(has_below, 1, 0) + jnp.where(has_above2, 1, 0) + jnp.where(has_below2, 1, 0)
    )
    pl.semaphore_wait(barrier, neighbours)
    xcopies = [
        (has_right, has_left, remote(to_right, from_left, xs_sem.at[0], xr_sem.at[0], (g, right))),
        (has_left, has_right, remote(to_left, from_right, xs_sem.at[1], xr_sem.at[1], (g, left))),
    ]
    start(xcopies)

    for l in range(LEVELS):
        n = NZ >> l
        r = dot(ayv[l], stacked(jnp.concatenate([own[l][p] for p in range(n)], axis=1)))
        tail = [r[BY:, p * BX : (p + 1) * BX] for p in range(n)]
        for p in range(n):
            yo[OFF[l] + p] = r[:BY, p * BX : (p + 1) * BX]
            if l == 0:
                send0[0, p] = tail[p][:4]
                send0[1, p] = tail[p][12:]
        for first in range(0, n, 1 << l) if l else ():
            both = tail[first]
            for p in range(first + 1, min(first + (1 << l), n)):
                both = both + pltpu.roll(tail[p], p - first, 1)
            send1[0, SLOT[l] + (first >> l)] = both[:8]
            send1[1, SLOT[l] + (first >> l)] = both[8:]
    y1copies = [
        (has_below, has_above, remote(send0.at[0], recv0.at[0], ys_sem.at[0], yr_sem.at[0], (below, t))),
        (has_above, has_below, remote(send0.at[1], recv0.at[1], ys_sem.at[1], yr_sem.at[1], (above, t))),
        (has_below, has_above, remote(send1.at[0], recv1.at[0], ys_sem.at[2], yr_sem.at[2], (below, t))),
        (has_above, has_below, remote(send1.at[1], recv1.at[1], ys_sem.at[3], yr_sem.at[3], (above, t))),
        (has_below2, has_above2, remote(send1.at[0, SLOT[3]], recv2, ys_sem.at[4], yr_sem.at[4], (below2, t))),
    ]
    start(y1copies)

    finish(xcopies)
    w = lanes_of((8, BX))
    middle = jnp.where(w % 8 < 4, from_left[24:32], from_right[24:32])
    for k in range(2):
        send2[k, 0] = middle
        send2[k, 1] = from_left[56 + 8 * k : 64 + 8 * k]
        send2[k, 2] = from_right[56 + 8 * k : 64 + 8 * k]
    y2copies = [
        (has_below, has_above, remote(send2.at[0], recv3.at[0], ys_sem.at[5], yr_sem.at[5], (below, t))),
        (has_above, has_below, remote(send2.at[1], recv3.at[1], ys_sem.at[6], yr_sem.at[6], (above, t))),
        (has_below2, has_above2, remote(send2.at[0], recv4, ys_sem.at[7], yr_sem.at[7], (below2, t))),
    ]
    start(y2copies)

    def spread(l, p, packed0, packed_r, packed_l):
        win = 8 << l
        turned = lambda e, s: pltpu.roll(e, (-s) % BX, 1)
        if l == 0:
            return jnp.where((lanes_of(packed0.shape) + 4) % BX < 8, turned(packed0, 8 * p), 0.0)
        w = lanes_of(packed_r.shape)
        a = jnp.where(w < win, turned(packed_r, win * p + SR[l]), 0.0)
        return a + jnp.where(w >= BX - win, turned(packed_l, win * p + SL[l]), 0.0)

    a, b = from_left[:24], from_right[:24]
    w = lanes_of((24, BX)) % 8 < 4
    wide[0, 0, :24] = jnp.where(w, a, b)
    wide[0, 0, 24:] = jnp.where(w, pltpu.roll(a, BX - 4, 1), pltpu.roll(b, 4, 1))
    for l in range(1, LEVELS):
        n = BY >> l
        wide[l, 0, pl.ds(0, n, stride=1 << l), :] = from_left[32 : 32 + n]
        wide[l, 1, pl.ds(0, n, stride=1 << l), :] = from_right[32 : 32 + n]

    row = lax.broadcasted_iota(jnp.int32, (BY, BX), 0)
    for z in range(NZ):
        value = None
        for l in reversed(range(LEVELS)):
            if z % (1 << l):
                continue
            p = z >> l
            part = yo[OFF[l] + p] + spread(l, p, wide[l, 0], wide[l, 0], wide[l, 1])
            if value is None:
                value = part
            else:
                step = 2 << l
                value = jnp.where((row % step == 0) & (lane % step == 0), value, part)
        yo[z] = value

    finish(y1copies)
    finish(y2copies)
    lane = lanes_of((1, BX))
    outer = [jnp.concatenate([recv3[0, k], recv3[1, k]], axis=0) for k in range(3)]

    def valid(l, p, j, v):
        if l and p % 2 == 0 and j % 2 == 0 and l < LEVELS - 1:
            return jnp.where(lane % (2 << l) == 1 << l, v, 0.0)
        if l:
            return jnp.where(lane % (1 << l) == 0, v, 0.0)
        if p % 2 == 0 and j % 2 == 0:
            return jnp.where(lane % 2 == 1, v, 0.0)
        return v

    for z in range(NZ):
        adds = {}
        for l in range(LEVELS):
            if z % (1 << l):
                continue
            p = z >> l
            e = spread(l, p, *outer)
            if l == 0:
                down, up = recv0[0, p] + e[:4], recv0[1, p] + e[12:]
            else:
                slot, turn = SLOT[l] + (p >> l), (BX - p % (1 << l)) % BX
                down = pltpu.roll(recv1[0, slot], turn, 1) + e[:8]
                up = pltpu.roll(recv1[1, slot], turn, 1) + e[8:]
            for k in range(3 if l == 0 else 7):
                if k << l < BY:
                    adds.setdefault(k << l, []).append(valid(l, p, k, down[k : k + 1]))
            for k in range(4 if l == 0 else 2, 8):
                adds.setdefault(BY - ((8 - k) << l), []).append(valid(l, p, k, up[k - 4 : k - 3] if l == 0 else up[k : k + 1]))
            if l == 3:
                v = pltpu.roll(recv2[...], turn, 1) + spread(l, p, None, recv4[1], recv4[2])
                adds[0].append(valid(l, p, 6, v[6:7]))
        for r, vs in adds.items():
            yo[z, r : r + 1, :] = functools.reduce(lambda a, b: a + b, vs, yo[z, r : r + 1, :])
        out_ref[z] = yo[z].astype(BF16)


def body(quantized, scales):
    groups, tiles = lax.axis_size("grp"), lax.axis_size("tile")
    hbm = pl.BlockSpec(memory_space=pl.ANY)
    dma = pltpu.SemaphoreType.DMA
    return pl.pallas_call(
        functools.partial(kernel, groups, tiles),
        out_shape=pltpu.VMEM((NZ, BY, BX), BF16),
        in_specs=[hbm] * 5,

        scratch_shapes=[
            pltpu.VMEM((NZ, BY, BX), BF16),
            pltpu.VMEM((1, NZ, BY), F32),
            pltpu.VMEM((LEVELS, 2 * BX, 2 * BX), BF16),
            pltpu.VMEM((LEVELS, BY + 16, 3 * BY), BF16),
            pltpu.VMEM((LEVELS - 1, 40, 3 * BY), BF16),
            pltpu.VMEM((NP, BY, BX), BF16),
            pltpu.VMEM((NP, BY, BX), BF16),
            pltpu.VMEM((72, BX), F32),
            pltpu.VMEM((72, BX), F32),
            pltpu.VMEM((72, BX), F32),
            pltpu.VMEM((72, BX), F32),
            pltpu.VMEM((LEVELS, 2, BY, BX), F32),
            pltpu.VMEM((NP, BY, BX), F32),
            pltpu.VMEM((2, NZ, 4, BX), F32),
            pltpu.VMEM((2, 6, 8, BX), F32),
            pltpu.VMEM((2, 3, 8, BX), F32),
            pltpu.VMEM((2, NZ, 4, BX), F32),
            pltpu.VMEM((2, 6, 8, BX), F32),
            pltpu.VMEM((8, BX), F32),
            pltpu.VMEM((2, 3, 8, BX), F32),
            pltpu.VMEM((3, 8, BX), F32),
            dma((5,)), dma((2,)), dma((2,)), dma((8,)), dma((8,)),
        ],
        compiler_params=pltpu.CompilerParams(collective_id=0, has_side_effects=True),
    )(quantized, scales, jnp.asarray(x_matrices()), jnp.asarray(y_matrices(groups)),
      jnp.asarray(packed_matrices(groups)))


def solution(mesh):
    return jax.shard_map(
        body,
        mesh=mesh,
        in_specs=(P(None, "grp", "tile"), P("tile", None, "grp")),
        out_specs=P(None, "grp", "tile"),
        check_vma=False,
    )
```

```python
import functools

import jax
import jax.numpy as jnp
import numpy as np
from jax import lax
from jax.experimental import pallas as pl
from jax.experimental.pallas import tpu as pltpu
from jax.sharding import PartitionSpec as P

LEVELS = 4
ALPHA = -1.586134342059924
BETA = -0.052980118572961
GAMMA = 0.882911075530934
DELTA = 0.443506852043971
KAPPA = 1.230174104914001

NZ, BY, BX = 16, 48, 128
OFF = (0, 16, 24, 28)
NP = 30
SR = (0, 0, 1, 3)
SL = (0, 1, 2, 0)
SLOT = (0, 0, 4, 5)
MESH = pl.DeviceIdType.MESH
F32, BF16 = jnp.float32, jnp.bfloat16


def lift_list(v):
    e, o = list(v[0::2]), list(v[1::2])
    m = len(e)
    up = lambda s: [s[min(i + 1, m - 1)] for i in range(m)]
    down = lambda s: [s[max(i - 1, 0)] for i in range(m)]
    o = [x + ALPHA * (a + b) for x, a, b in zip(o, e, up(e))]
    e = [x + BETA * (a + b) for x, a, b in zip(e, down(o), o)]
    o = [x + GAMMA * (a + b) for x, a, b in zip(o, e, up(e))]
    e = [x + DELTA * (a + b) for x, a, b in zip(e, down(o), o)]
    e = [x * (1.0 / KAPPA) for x in e]
    o = [x * (KAPPA / 2.0) for x in o]
    return [x for pair in zip(e, o) for x in pair]


def level_matrices(n):
    low, out = np.eye(n), []
    for _ in range(LEVELS):
        full = np.stack(lift_list(list(low)))
        out.append(full)
        low = full[::2]
    return out


def split(a):
    hi = a.astype(np.float32).astype(BF16)
    lo = (a - hi.astype(np.float64)).astype(np.float32).astype(BF16)
    return hi, lo


def hi_hi_lo(a):
    hi, lo = split(a)
    return np.concatenate([hi, hi, lo], axis=-1)


@functools.cache
def x_matrices():
    w = level_matrices(3 * BX)
    m = np.zeros((3, LEVELS, BX, 2 * BX))
    for v in range(3):
        for l in range(LEVELS):
            b, win = BX >> l, 8 << l
            mine = w[l][:, v * BX : (v + 1) * BX]
            for j in range(b):
                m[v, l, :, j << l] = mine[v * b + j]
            for start in range(0, BX, win):
                if v < 2:
                    for j in range(4 if l == 0 else 7):
                        lane = start + (j << l) + SR[l]
                        if j << l < win:
                            m[v, l, :, BX + lane] = mine[(v + 1) * b + j]
                if v > 0:
                    for j in range(1, 5 if l == 0 else 7):
                        lane = (start - (j << l) + SL[l]) % BX
                        m[v, l, :, BX + lane] = mine[v * b - j]
    hi, lo = split(m)
    return np.concatenate([hi, lo], axis=2)


@functools.cache
def y_matrices(groups):
    n = groups * BY
    w = level_matrices(n)
    m = np.zeros((groups, LEVELS, BY + 16, BY))
    for g in range(groups):
        for l in range(LEVELS):
            b = BY >> l
            mine = w[l][:, g * BY : (g + 1) * BY]
            for j in range(b):
                m[g, l, j << l] = mine[g * b + j]
            for k in range(8):
                r = (g + 1) * b + k
                if r < n >> l:
                    m[g, l, BY + k] = mine[r]
                r = g * b - 8 + k
                if r >= max((g - 1) * b, 0):
                    m[g, l, BY + 8 + k] = mine[r]
    return hi_hi_lo(m)


@functools.cache
def packed_matrices(groups):
    m = y_matrices(groups)
    out = np.zeros((groups, LEVELS - 1, 40, 3 * BY), m.dtype)
    for l in range(1, LEVELS):
        out[:, l - 1, : BY >> l] = m[:, l, : BY : 1 << l]
        out[:, l - 1, 24:] = m[:, l, BY:]
    return out


def hilo(x):
    hi = x.astype(BF16)
    return hi, (x - hi.astype(F32)).astype(BF16)


def stacked(x):
    hi, lo = hilo(x)
    return jnp.concatenate([hi, lo, hi], axis=0)


def dot(a, b):
    return jnp.dot(a, b, preferred_element_type=F32)


def lanes_of(shape):
    return lax.broadcasted_iota(jnp.int32, shape, len(shape) - 1)


def kernel(
    groups, tiles,
    q_hbm, s_hbm, mx_hbm, ay_hbm, ac_hbm, out_ref,
    qv, sv, mxv, ayv, acv, zh, zl, to_right, to_left, from_left, from_right,
    to_right_far, to_left_far, from_left_far, from_right_far, wide, wide2, yo,
    send0, send1, recv0, recv1, recv2, down2, up2, down3,
    load_sem, xs_sem, xr_sem, ys_sem, yr_sem,
):
    g, t = lax.axis_index("grp"), lax.axis_index("tile")
    right, left = lax.rem(t + 1, tiles), lax.rem(t + tiles - 1, tiles)
    below, above = lax.rem(g + 1, groups), lax.rem(g + groups - 1, groups)
    below2, above2 = lax.rem(g + 2, groups), lax.rem(g + groups - 2, groups)

    has_left, has_right = t > 0, t < tiles - 1
    has_above, has_below = g > 0, g < groups - 1
    has_above2, has_below2 = g > 1, g < groups - 2
    barrier = pltpu.get_barrier_semaphore()
    for there, dev in (
        (has_left, (g, left)), (has_right, (g, right)),
        (has_above, (above, t)), (has_below, (below, t)),
        (has_above2, (above2, t)), (has_below2, (below2, t)),
    ):
        @pl.when(there)
        def _():
            pl.semaphore_signal(barrier, inc=1, device_id=dev, device_id_type=MESH)

    side = jnp.where(t == 0, 0, jnp.where(t == tiles - 1, 2, 1))
    loads = [
        pltpu.make_async_copy(q_hbm, qv, load_sem.at[0]),
        pltpu.make_async_copy(s_hbm, sv, load_sem.at[1]),
        pltpu.make_async_copy(mx_hbm.at[side], mxv, load_sem.at[2]),
        pltpu.make_async_copy(ay_hbm.at[g], ayv, load_sem.at[3]),
        pltpu.make_async_copy(ac_hbm.at[g], acv, load_sem.at[4]),
    ]
    for c in loads:
        c.start()
    for there, buffers in (
        (has_left, (from_left, from_left_far)),
        (has_right, (from_right, from_right_far)),
        (has_above, (recv0.at[0], recv1.at[0], down2)),
        (has_below, (recv0.at[1], recv1.at[1], up2)),
        (has_above2, (recv2, down3)),
    ):
        @pl.when(jnp.logical_not(there))
        def _():
            for b in buffers:
                b[...] = jnp.zeros(b.shape, F32)
    loads[1].wait()
    loads[0].wait()

    st = jnp.transpose(sv[0])
    for c in range(3):
        rows = slice(16 * c, 16 * c + 16)
        band = [qv[z, rows, :].astype(F32) * st[rows, z : z + 1] for z in range(NZ)]
        for l in range(LEVELS):
            band = lift_list(band)
            for p, v in enumerate(band):
                hi, lo = hilo(v)
                zh[OFF[l] + p, rows, :] = hi
                zl[OFF[l] + p, rows, :] = lo
            band = band[0::2]

    loads[2].wait()
    own, packs = [], []
    lane = lanes_of((1, 1, BX))
    for l in range(LEVELS):
        n, win = NZ >> l, 8 << l
        h = zh[OFF[l] : OFF[l] + n].reshape(n * BY, BX)
        low = zl[OFF[l] : OFF[l] + n].reshape(n * BY, BX)
        mh, ml = mxv[l, :BX], mxv[l, BX:]
        r = dot(jnp.concatenate([h, low, h], axis=1), jnp.concatenate([mh, mh, ml], axis=0))
        own.append(r[:, :BX].reshape(n, BY, BX))
        if l == 0:
            plane = ((lane + 4) // 8) % NZ
        else:
            rightward = (lane % (1 << l)) == SR[l] % (1 << l)
            plane = jnp.where(rightward, lane // win, (lane // win + 1) % n)
        which = lax.broadcasted_iota(jnp.int32, (n, 1, BX), 0)
        packs.append(jnp.sum(jnp.where(which == plane, r[:, BX:].reshape(n, BY, BX), 0.0), axis=0))

    loads[3].wait()
    loads[4].wait()
    e0 = dot(ayv[0], stacked(packs[0]))
    e1, e2, e3 = (dot(acv[l - 1], stacked(packs[l])) for l in range(1, LEVELS))
    lane = lanes_of((40, BX))
    rightward = jnp.where(lane % 2 == 0, e1, jnp.where(lane % 4 == 1, e2, e3))
    leftward = jnp.where(lane % 2 == 1, e1, jnp.where(lane % 4 == 2, e2, e3))
    for far, v in ((to_right_far, rightward), (to_left_far, leftward)):
        far[:8] = v[24:32]
        far[8:16] = e0[48:56] + e0[56:]
        far[16:] = v[32:]
    lane = lanes_of((24, BX))
    to_right[:24] = jnp.where(lane % 8 < 4, e0[:24], pltpu.roll(e0[24:48], 4, 1))
    to_left[:24] = jnp.where(lane % 8 >= 4, e0[:24], pltpu.roll(e0[24:48], BX - 4, 1))
    to_right[24:] = rightward[:24]
    to_left[24:] = leftward[:24]
    lane = lanes_of((BY, BX))

    def remote(src, dst, ss, rs, dev):
        return pltpu.make_async_remote_copy(
            src_ref=src, dst_ref=dst, send_sem=ss, recv_sem=rs, device_id=dev, device_id_type=MESH
        )

    def start(copies):
        for to, _, c in copies:
            pl.when(to)(c.start)

    def finish(copies):
        for to, came, c in copies:
            pl.when(came)(c.wait_recv)
        for to, came, c in copies:
            pl.when(to)(c.wait_send)

    neighbours = (
        jnp.where(has_left, 1, 0) + jnp.where(has_right, 1, 0) + jnp.where(has_above, 1, 0)
        + jnp.where(has_below, 1, 0) + jnp.where(has_above2, 1, 0) + jnp.where(has_below2, 1, 0)
    )
    pl.semaphore_wait(barrier, neighbours)
    farcopies = [
        (has_right, has_left, remote(to_right_far, from_left_far, xs_sem.at[0], xr_sem.at[0], (g, right))),
        (has_left, has_right, remote(to_left_far, from_right_far, xs_sem.at[1], xr_sem.at[1], (g, left))),
    ]
    start(farcopies)
    xcopies = [
        (has_right, has_left, remote(to_right, from_left, xs_sem.at[2], xr_sem.at[2], (g, right))),
        (has_left, has_right, remote(to_left, from_right, xs_sem.at[3], xr_sem.at[3], (g, left))),
    ]
    start(xcopies)

    for l in range(LEVELS):
        n = NZ >> l
        r = dot(ayv[l], stacked(jnp.concatenate([own[l][p] for p in range(n)], axis=1)))
        tail = [r[BY:, p * BX : (p + 1) * BX] for p in range(n)]
        for p in range(n):
            yo[OFF[l] + p] = r[:BY, p * BX : (p + 1) * BX]
            if l == 0:
                send0[0, p] = tail[p][:4]
                send0[1, p] = tail[p][12:]
        for first in range(0, n, 1 << l) if l else ():
            both = tail[first]
            for p in range(first + 1, min(first + (1 << l), n)):
                both = both + pltpu.roll(tail[p], p - first, 1)
            send1[0, SLOT[l] + (first >> l)] = both[:8]
            send1[1, SLOT[l] + (first >> l)] = both[8:]
    y1copies = [
        (has_below, has_above, remote(send0.at[0], recv0.at[0], ys_sem.at[0], yr_sem.at[0], (below, t))),
        (has_above, has_below, remote(send0.at[1], recv0.at[1], ys_sem.at[1], yr_sem.at[1], (above, t))),
        (has_below, has_above, remote(send1.at[0], recv1.at[0], ys_sem.at[2], yr_sem.at[2], (below, t))),
        (has_above, has_below, remote(send1.at[1], recv1.at[1], ys_sem.at[3], yr_sem.at[3], (above, t))),
        (has_below2, has_above2, remote(send1.at[0, SLOT[3]], recv2, ys_sem.at[4], yr_sem.at[4], (below2, t))),
    ]
    start(y1copies)

    finish(farcopies)
    y2copies = []
    for k, far in enumerate((from_left_far, from_right_far)):
        y2copies += [
            (has_below, has_above, remote(far.at[:16], down2.at[k], ys_sem.at[5 + k], yr_sem.at[5 + k], (below, t))),
            (has_above, has_below, remote(far.at[8:], up2.at[k], ys_sem.at[7 + k], yr_sem.at[7 + k], (above, t))),
            (has_below2, has_above2, remote(far.at[:8], down3.at[k], ys_sem.at[9 + k], yr_sem.at[9 + k], (below2, t))),
        ]
    start(y2copies)

    def spread(l, p, packed0, packed_r, packed_l, keep=None):
        win = 8 << l
        turned = lambda e, s: pltpu.roll(e, (-s) % BX, 1)
        both = (lambda m: m) if keep is None else (lambda m: jnp.logical_and(m, keep))
        if l == 0:
            return jnp.where(both((lanes_of(packed0.shape) + 4) % BX < 8), turned(packed0, 8 * p), 0.0)
        w = lanes_of(packed_r.shape)
        a = jnp.where(both(w < win), turned(packed_r, win * p + SR[l]), 0.0)
        return a + jnp.where(both(w >= BX - win), turned(packed_l, win * p + SL[l]), 0.0)

    finish(xcopies)
    a, b = from_left[:24], from_right[:24]
    w = lanes_of((24, BX)) % 8 < 4
    wide[0, 0, :24] = jnp.where(w, a, b)
    wide[0, 0, 24:] = jnp.where(w, pltpu.roll(a, BX - 4, 1), pltpu.roll(b, 4, 1))
    for l in range(1, LEVELS):
        n = BY >> l
        wide[l, 0, pl.ds(0, n, stride=1 << l), :] = from_left[24 : 24 + n]
        wide[l, 1, pl.ds(0, n, stride=1 << l), :] = from_right[24 : 24 + n]

    row = lax.broadcasted_iota(jnp.int32, (BY, BX), 0)
    for z in range(NZ):
        value = None
        for l in reversed(range(LEVELS)):
            if z % (1 << l):
                continue
            p = z >> l
            part = yo[OFF[l] + p] + spread(l, p, wide[l, 0], wide[l, 0], wide[l, 1])
            if value is None:
                value = part
            else:
                step = 2 << l
                value = jnp.where((row % step == 0) & (lane % step == 0), value, part)
        yo[z] = value

    wide2[...] = jnp.zeros(wide2.shape, F32)
    finish(y1copies)
    lane = lanes_of((1, BX))

    def valid(l, p, j, v):
        if l and p % 2 == 0 and j % 2 == 0 and l < LEVELS - 1:
            return jnp.where(lane % (2 << l) == 1 << l, v, 0.0)
        if l:
            return jnp.where(lane % (1 << l) == 0, v, 0.0)
        if p % 2 == 0 and j % 2 == 0:
            return jnp.where(lane % 2 == 1, v, 0.0)
        return v

    for z in range(NZ):
        adds = {}
        for l in range(LEVELS):
            if z % (1 << l):
                continue
            p = z >> l
            if l == 0:
                down, up = recv0[0, p], recv0[1, p]
            else:
                slot, turn = SLOT[l] + (p >> l), (BX - p % (1 << l)) % BX
                down = pltpu.roll(recv1[0, slot], turn, 1)
                up = pltpu.roll(recv1[1, slot], turn, 1)
            for k in range(3 if l == 0 else 7):
                if k << l < BY:
                    adds.setdefault(k << l, []).append(valid(l, p, k, down[k : k + 1]))
            for k in range(4 if l == 0 else 2, 8):
                adds.setdefault(BY - ((8 - k) << l), []).append(valid(l, p, k, up[k - 4 : k - 3] if l == 0 else up[k : k + 1]))
            if l == 3:
                v = pltpu.roll(recv2[...], turn, 1)
                adds[0].append(valid(l, p, 6, v[6:7]))
        for r, vs in adds.items():
            yo[z, r : r + 1, :] = functools.reduce(lambda a, b: a + b, vs, yo[z, r : r + 1, :])

    finish(y2copies)
    for k in range(2):
        for l in range(1, LEVELS):
            n, rows = min(7, BY >> l), wide2.at[l - 1, k]
            rows[pl.ds(0, n, stride=1 << l), :] = down2[k, :n]
            last = pl.ds(BY - (6 << l), 6, stride=1 << l)
            rows[last, :] = rows[last, :] + up2[k, 10:]
        wide2[2, k, 0:1] = wide2[2, k, 0:1] + down3[k, 6:7]
    w, r = lanes_of((8, BX)), lax.broadcasted_iota(jnp.int32, (8, BX), 0)
    top = jnp.where(w % 8 < 4, down2[0, 8:], down2[1, 8:])
    low = jnp.where(w % 8 < 4, up2[0, :8], up2[1, :8])
    ends = jnp.where(r < 4, top, low)
    not_lower = jnp.logical_or(r % 2 == 1, w % 2 == 1)
    for z in range(NZ):
        tiles = [yo[z, 8 * i : 8 * i + 8, :] for i in range(6)]
        e = spread(0, z, ends, None, None, not_lower if z % 2 == 0 else None)
        tiles[0] = tiles[0] + jnp.where(r < 4, e, 0.0)
        tiles[5] = tiles[5] + jnp.where(r < 4, 0.0, e)
        for l in range(1, LEVELS):
            if z % (1 << l):
                continue
            p = z >> l
            for i in (0, 1, 4, 5) if l == 1 else range(6):
                keep = w % (1 << l) == 0
                if p % 2 == 0 and l < LEVELS - 1:
                    keep = jnp.logical_and(keep, jnp.logical_or(r % (2 << l) > 0, w % (2 << l) > 0))
                a, b = (wide2[l - 1, k, 8 * i : 8 * i + 8, :] for k in range(2))
                tiles[i] = tiles[i] + spread(l, p, None, a, b, keep)
        out_ref[z] = jnp.concatenate(tiles, axis=0).astype(BF16)


def body(quantized, scales):
    groups, tiles = lax.axis_size("grp"), lax.axis_size("tile")
    hbm = pl.BlockSpec(memory_space=pl.ANY)
    dma = pltpu.SemaphoreType.DMA
    return pl.pallas_call(
        functools.partial(kernel, groups, tiles),
        out_shape=pltpu.VMEM((NZ, BY, BX), BF16),
        in_specs=[hbm] * 5,

        scratch_shapes=[
            pltpu.VMEM((NZ, BY, BX), BF16),
            pltpu.VMEM((1, NZ, BY), F32),
            pltpu.VMEM((LEVELS, 2 * BX, 2 * BX), BF16),
            pltpu.VMEM((LEVELS, BY + 16, 3 * BY), BF16),
            pltpu.VMEM((LEVELS - 1, 40, 3 * BY), BF16),
            pltpu.VMEM((NP, BY, BX), BF16),
            pltpu.VMEM((NP, BY, BX), BF16),
            *[pltpu.VMEM((BY, BX), F32) for _ in range(4)],
            *[pltpu.VMEM((24, BX), F32) for _ in range(4)],
            pltpu.VMEM((LEVELS, 2, BY, BX), F32),
            pltpu.VMEM((LEVELS - 1, 2, BY, BX), F32),
            pltpu.VMEM((NP, BY, BX), F32),
            pltpu.VMEM((2, NZ, 4, BX), F32),
            pltpu.VMEM((2, 6, 8, BX), F32),
            pltpu.VMEM((2, NZ, 4, BX), F32),
            pltpu.VMEM((2, 6, 8, BX), F32),
            pltpu.VMEM((8, BX), F32),
            pltpu.VMEM((2, 16, BX), F32),
            pltpu.VMEM((2, 16, BX), F32),
            pltpu.VMEM((2, 8, BX), F32),
            dma((5,)), dma((4,)), dma((4,)), dma((11,)), dma((11,)),
        ],
        compiler_params=pltpu.CompilerParams(collective_id=0, has_side_effects=True),
    )(quantized, scales, jnp.asarray(x_matrices()), jnp.asarray(y_matrices(groups)),
      jnp.asarray(packed_matrices(groups)))


def solution(mesh):
    return jax.shard_map(
        body,
        mesh=mesh,
        in_specs=(P(None, "grp", "tile"), P("tile", None, "grp")),
        out_specs=P(None, "grp", "tile"),
        check_vma=False,
    )
```

```python
import functools

import jax
import jax.numpy as jnp
import numpy as np
from jax import lax
from jax.experimental import pallas as pl
from jax.experimental.pallas import tpu as pltpu
from jax.sharding import PartitionSpec as P

LEVELS = 4
ALPHA = -1.586134342059924
BETA = -0.052980118572961
GAMMA = 0.882911075530934
DELTA = 0.443506852043971
KAPPA = 1.230174104914001

NZ, BY, BX = 16, 48, 128
OFF = (0, 16, 24, 28)
NP = 30
SR = (0, 0, 1, 3)
SL = (0, 1, 2, 0)
SLOT = (0, 0, 4, 5)
MESH = pl.DeviceIdType.MESH
F32, BF16 = jnp.float32, jnp.bfloat16


def lift_list(v):
    e, o = list(v[0::2]), list(v[1::2])
    m = len(e)
    up = lambda s: [s[min(i + 1, m - 1)] for i in range(m)]
    down = lambda s: [s[max(i - 1, 0)] for i in range(m)]
    o = [x + ALPHA * (a + b) for x, a, b in zip(o, e, up(e))]
    e = [x + BETA * (a + b) for x, a, b in zip(e, down(o), o)]
    o = [x + GAMMA * (a + b) for x, a, b in zip(o, e, up(e))]
    e = [x + DELTA * (a + b) for x, a, b in zip(e, down(o), o)]
    e = [x * (1.0 / KAPPA) for x in e]
    o = [x * (KAPPA / 2.0) for x in o]
    return [x for pair in zip(e, o) for x in pair]


def level_matrices(n):
    low, out = np.eye(n), []
    for _ in range(LEVELS):
        full = np.stack(lift_list(list(low)))
        out.append(full)
        low = full[::2]
    return out


def split(a):
    hi = a.astype(np.float32).astype(BF16)
    lo = (a - hi.astype(np.float64)).astype(np.float32).astype(BF16)
    return hi, lo


def hi_hi_lo(a):
    hi, lo = split(a)
    return np.concatenate([hi, hi, lo], axis=-1)


@functools.cache
def x_matrices():
    w = level_matrices(3 * BX)
    m = np.zeros((3, LEVELS, BX, 2 * BX))
    for v in range(3):
        for l in range(LEVELS):
            b, win = BX >> l, 8 << l
            mine = w[l][:, v * BX : (v + 1) * BX]
            for j in range(b):
                m[v, l, :, j << l] = mine[v * b + j]
            for start in range(0, BX, win):
                if v < 2:
                    for j in range(4 if l == 0 else 7):
                        lane = start + (j << l) + SR[l]
                        if j << l < win:
                            m[v, l, :, BX + lane] = mine[(v + 1) * b + j]
                if v > 0:
                    for j in range(1, 5 if l == 0 else 7):
                        lane = (start - (j << l) + SL[l]) % BX
                        m[v, l, :, BX + lane] = mine[v * b - j]
    hi, lo = split(m)
    return np.concatenate([hi, lo], axis=2)


@functools.cache
def y_matrices(groups):
    n = groups * BY
    w = level_matrices(n)
    m = np.zeros((groups, LEVELS, BY + 16, BY))
    for g in range(groups):
        for l in range(LEVELS):
            b = BY >> l
            mine = w[l][:, g * BY : (g + 1) * BY]
            for j in range(b):
                m[g, l, j << l] = mine[g * b + j]
            for k in range(8):
                r = (g + 1) * b + k
                if r < n >> l:
                    m[g, l, BY + k] = mine[r]
                r = g * b - 8 + k
                if r >= max((g - 1) * b, 0):
                    m[g, l, BY + 8 + k] = mine[r]
    return hi_hi_lo(m)


@functools.cache
def packed_matrices(groups):
    m = y_matrices(groups)
    out = np.zeros((groups, LEVELS - 1, 40, 3 * BY), m.dtype)
    for l in range(1, LEVELS):
        out[:, l - 1, : BY >> l] = m[:, l, : BY : 1 << l]
        out[:, l - 1, 24:] = m[:, l, BY:]
    return out


def hilo(x):
    hi = x.astype(BF16)
    return hi, (x - hi.astype(F32)).astype(BF16)


def stacked(x):
    hi, lo = hilo(x)
    return jnp.concatenate([hi, lo, hi], axis=0)


def dot(a, b):
    return jnp.dot(a, b, preferred_element_type=F32)


def lanes_of(shape):
    return lax.broadcasted_iota(jnp.int32, shape, len(shape) - 1)


def kernel(
    groups, tiles,
    q_hbm, s_hbm, mx_hbm, ay_hbm, ac_hbm, out_ref,
    qv, sv, mxv, ayv, acv, zh, zl, to_right, to_left, from_left, from_right,
    to_right_far, to_left_far, from_left_far, from_right_far, wide, wide2, yo,
    send0, send1, recv0, recv1, recv2, down2, up2, down3,
    pass_down, pass_up, pass_down2,
    load_sem, xs_sem, xr_sem, ys_sem, yr_sem, ps_sem, pr_sem,
):
    g, t = lax.axis_index("grp"), lax.axis_index("tile")
    right, left = lax.rem(t + 1, tiles), lax.rem(t + tiles - 1, tiles)
    below, above = lax.rem(g + 1, groups), lax.rem(g + groups - 1, groups)
    below2, above2 = lax.rem(g + 2, groups), lax.rem(g + groups - 2, groups)

    has_left, has_right = t > 0, t < tiles - 1
    has_above, has_below = g > 0, g < groups - 1
    has_above2, has_below2 = g > 1, g < groups - 2
    odd = lax.rem(t, 2) == 1
    even = jnp.logical_not(odd)
    also = lambda *conditions: functools.reduce(jnp.logical_and, conditions)
    barrier = pltpu.get_barrier_semaphore()
    for there, dev in (
        (has_left, (g, left)), (has_right, (g, right)),
        (has_above, (above, t)), (has_below, (below, t)),
        (has_above2, (above2, t)), (has_below2, (below2, t)),
    ):
        @pl.when(there)
        def _():
            pl.semaphore_signal(barrier, inc=1, device_id=dev, device_id_type=MESH)

    side = jnp.where(t == 0, 0, jnp.where(t == tiles - 1, 2, 1))
    loads = [
        pltpu.make_async_copy(q_hbm, qv, load_sem.at[0]),
        pltpu.make_async_copy(s_hbm, sv, load_sem.at[1]),
        pltpu.make_async_copy(mx_hbm.at[side], mxv, load_sem.at[2]),
        pltpu.make_async_copy(ay_hbm.at[g], ayv, load_sem.at[3]),
        pltpu.make_async_copy(ac_hbm.at[g], acv, load_sem.at[4]),
    ]
    for c in loads:
        c.start()
    for there, buffers in (
        (has_left, (from_left, from_left_far)),
        (has_right, (from_right, from_right_far)),
        (has_above, (recv0.at[0], recv1.at[0], down2)),
        (has_below, (recv0.at[1], recv1.at[1], up2)),
        (has_above2, (recv2, down3)),
        (jnp.logical_or(odd, has_left), (down2.at[0], up2.at[0], down3.at[0])),
    ):
        @pl.when(jnp.logical_not(there))
        def _():
            for b in buffers:
                b[...] = jnp.zeros(b.shape, F32)
    loads[1].wait()
    loads[0].wait()

    st = jnp.transpose(sv[0])
    for c in range(3):
        rows = slice(16 * c, 16 * c + 16)
        band = [qv[z, rows, :].astype(F32) * st[rows, z : z + 1] for z in range(NZ)]
        for l in range(LEVELS):
            band = lift_list(band)
            for p, v in enumerate(band):
                hi, lo = hilo(v)
                zh[OFF[l] + p, rows, :] = hi
                zl[OFF[l] + p, rows, :] = lo
            band = band[0::2]

    loads[2].wait()
    own, packs = [], []
    lane = lanes_of((1, 1, BX))
    for l in range(LEVELS):
        n, win = NZ >> l, 8 << l
        h = zh[OFF[l] : OFF[l] + n].reshape(n * BY, BX)
        low = zl[OFF[l] : OFF[l] + n].reshape(n * BY, BX)
        mh, ml = mxv[l, :BX], mxv[l, BX:]
        r = dot(jnp.concatenate([h, low, h], axis=1), jnp.concatenate([mh, mh, ml], axis=0))
        own.append(r[:, :BX].reshape(n, BY, BX))
        if l == 0:
            plane = ((lane + 4) // 8) % NZ
        else:
            rightward = (lane % (1 << l)) == SR[l] % (1 << l)
            plane = jnp.where(rightward, lane // win, (lane // win + 1) % n)
        which = lax.broadcasted_iota(jnp.int32, (n, 1, BX), 0)
        packs.append(jnp.sum(jnp.where(which == plane, r[:, BX:].reshape(n, BY, BX), 0.0), axis=0))

    loads[3].wait()
    loads[4].wait()
    e0 = dot(ayv[0], stacked(packs[0]))
    e1, e2, e3 = (dot(acv[l - 1], stacked(packs[l])) for l in range(1, LEVELS))
    lane = lanes_of((40, BX))
    rightward = jnp.where(lane % 2 == 0, e1, jnp.where(lane % 4 == 1, e2, e3))
    leftward = jnp.where(lane % 2 == 1, e1, jnp.where(lane % 4 == 2, e2, e3))
    for far, v in ((to_right_far, rightward), (to_left_far, leftward)):
        far[:8] = v[24:32]
        far[8:16] = e0[48:56] + e0[56:]
        far[16:] = v[32:]
    lane = lanes_of((24, BX))
    to_right[:24] = jnp.where(lane % 8 < 4, e0[:24], pltpu.roll(e0[24:48], 4, 1))
    to_left[:24] = jnp.where(lane % 8 >= 4, e0[:24], pltpu.roll(e0[24:48], BX - 4, 1))
    to_right[24:] = rightward[:24]
    to_left[24:] = leftward[:24]
    lane = lanes_of((BY, BX))

    def remote(src, dst, ss, rs, dev):
        return pltpu.make_async_remote_copy(
            src_ref=src, dst_ref=dst, send_sem=ss, recv_sem=rs, device_id=dev, device_id_type=MESH
        )

    def start(copies):
        for to, _, c in copies:
            pl.when(to)(c.start)

    def arrived(copies):
        for _, came, c in copies:
            pl.when(came)(c.wait_recv)

    neighbours = (
        jnp.where(has_left, 1, 0) + jnp.where(has_right, 1, 0) + jnp.where(has_above, 1, 0)
        + jnp.where(has_below, 1, 0) + jnp.where(has_above2, 1, 0) + jnp.where(has_below2, 1, 0)
    )
    pl.semaphore_wait(barrier, neighbours)
    farcopies = [
        (also(even, has_right), also(odd, has_left), remote(to_right_far, from_left_far, xs_sem.at[0], xr_sem.at[0], (g, right))),
        (also(even, has_left), also(odd, has_right), remote(to_left_far, from_right_far, xs_sem.at[1], xr_sem.at[1], (g, left))),
    ]

    def along_y(k, far, down, up, down_2, send, recv, first):
        return [
            (also(odd, has_below), also(odd, has_above), remote(far.at[:16], down.at[k], send.at[first + k], recv.at[first + k], (below, t))),
            (also(odd, has_above), also(odd, has_below), remote(far.at[8:], up.at[k], send.at[first + 2 + k], recv.at[first + 2 + k], (above, t))),
            (also(odd, has_below2), also(odd, has_above2), remote(far.at[:8], down_2.at[k], send.at[first + 4 + k], recv.at[first + 4 + k], (below2, t))),
        ]

    own_far = [along_y(k, far, pass_down, pass_up, pass_down2, ps_sem, pr_sem, 0) for k, far in enumerate((to_right_far, to_left_far))]
    relays = [along_y(k, far, down2, up2, down3, ys_sem, yr_sem, 5) for k, far in enumerate((from_left_far, from_right_far))]
    forwards = []
    for k, to, came, dev in ((0, has_right, has_left, (g, right)), (1, has_left, has_right, (g, left))):
        forwards.append([
            (also(odd, to, there), also(even, came, there), remote(src.at[k], dst.at[k], ps_sem.at[6 + 2 * i + k], yr_sem.at[5 + 2 * i + k], dev))
            for i, (there, src, dst) in enumerate(((has_above, pass_down, down2), (has_below, pass_up, up2), (has_above2, pass_down2, down3)))
        ])
    start(own_far[0])
    start(own_far[1])
    start(farcopies)
    xcopies = [
        (has_right, has_left, remote(to_right, from_left, xs_sem.at[2], xr_sem.at[2], (g, right))),
        (has_left, has_right, remote(to_left, from_right, xs_sem.at[3], xr_sem.at[3], (g, left))),
    ]
    start(xcopies)

    for l in range(LEVELS):
        n = NZ >> l
        r = dot(ayv[l], stacked(jnp.concatenate([own[l][p] for p in range(n)], axis=1)))
        tail = [r[BY:, p * BX : (p + 1) * BX] for p in range(n)]
        for p in range(n):
            yo[OFF[l] + p] = r[:BY, p * BX : (p + 1) * BX]
            if l == 0:
                send0[0, p] = tail[p][:4]
                send0[1, p] = tail[p][12:]
        for first in range(0, n, 1 << l) if l else ():
            both = tail[first]
            for p in range(first + 1, min(first + (1 << l), n)):
                both = both + pltpu.roll(tail[p], p - first, 1)
            send1[0, SLOT[l] + (first >> l)] = both[:8]
            send1[1, SLOT[l] + (first >> l)] = both[8:]
    y1copies = [
        (has_below, has_above, remote(send0.at[0], recv0.at[0], ys_sem.at[0], yr_sem.at[0], (below, t))),
        (has_above, has_below, remote(send0.at[1], recv0.at[1], ys_sem.at[1], yr_sem.at[1], (above, t))),
        (has_below, has_above, remote(send1.at[0], recv1.at[0], ys_sem.at[2], yr_sem.at[2], (below, t))),
        (has_above, has_below, remote(send1.at[1], recv1.at[1], ys_sem.at[3], yr_sem.at[3], (above, t))),
        (has_below2, has_above2, remote(send1.at[0, SLOT[3]], recv2, ys_sem.at[4], yr_sem.at[4], (below2, t))),
    ]
    start(y1copies)

    arrived(farcopies[:1])
    start(relays[0])
    arrived(own_far[0])
    start(forwards[0])
    arrived(own_far[1])
    start(forwards[1])
    arrived(farcopies[1:])
    start(relays[1])

    def spread(l, p, packed0, packed_r, packed_l, keep=None):
        win = 8 << l
        turned = lambda e, s: pltpu.roll(e, (-s) % BX, 1)
        both = (lambda m: m) if keep is None else (lambda m: jnp.logical_and(m, keep))
        if l == 0:
            return jnp.where(both((lanes_of(packed0.shape) + 4) % BX < 8), turned(packed0, 8 * p), 0.0)
        w = lanes_of(packed_r.shape)
        a = jnp.where(both(w < win), turned(packed_r, win * p + SR[l]), 0.0)
        return a + jnp.where(both(w >= BX - win), turned(packed_l, win * p + SL[l]), 0.0)

    arrived(xcopies)
    a, b = from_left[:24], from_right[:24]
    w = lanes_of((24, BX)) % 8 < 4
    wide[0, 0, :24] = jnp.where(w, a, b)
    wide[0, 0, 24:] = jnp.where(w, pltpu.roll(a, BX - 4, 1), pltpu.roll(b, 4, 1))
    for l in range(1, LEVELS):
        n = BY >> l
        wide[l, 0, pl.ds(0, n, stride=1 << l), :] = from_left[24 : 24 + n]
        wide[l, 1, pl.ds(0, n, stride=1 << l), :] = from_right[24 : 24 + n]

    row = lax.broadcasted_iota(jnp.int32, (BY, BX), 0)
    for z in range(NZ):
        value = None
        for l in reversed(range(LEVELS)):
            if z % (1 << l):
                continue
            p = z >> l
            part = yo[OFF[l] + p] + spread(l, p, wide[l, 0], wide[l, 0], wide[l, 1])
            if value is None:
                value = part
            else:
                step = 2 << l
                value = jnp.where((row % step == 0) & (lane % step == 0), value, part)
        yo[z] = value

    wide2[...] = jnp.zeros(wide2.shape, F32)
    arrived(y1copies)
    lane = lanes_of((1, BX))

    def valid(l, p, j, v):
        if l and p % 2 == 0 and j % 2 == 0 and l < LEVELS - 1:
            return jnp.where(lane % (2 << l) == 1 << l, v, 0.0)
        if l:
            return jnp.where(lane % (1 << l) == 0, v, 0.0)
        if p % 2 == 0 and j % 2 == 0:
            return jnp.where(lane % 2 == 1, v, 0.0)
        return v

    for z in range(NZ):
        adds = {}
        for l in range(LEVELS):
            if z % (1 << l):
                continue
            p = z >> l
            if l == 0:
                down, up = recv0[0, p], recv0[1, p]
            else:
                slot, turn = SLOT[l] + (p >> l), (BX - p % (1 << l)) % BX
                down = pltpu.roll(recv1[0, slot], turn, 1)
                up = pltpu.roll(recv1[1, slot], turn, 1)
            for k in range(3 if l == 0 else 7):
                if k << l < BY:
                    adds.setdefault(k << l, []).append(valid(l, p, k, down[k : k + 1]))
            for k in range(4 if l == 0 else 2, 8):
                adds.setdefault(BY - ((8 - k) << l), []).append(valid(l, p, k, up[k - 4 : k - 3] if l == 0 else up[k : k + 1]))
            if l == 3:
                v = pltpu.roll(recv2[...], turn, 1)
                adds[0].append(valid(l, p, 6, v[6:7]))
        for r, vs in adds.items():
            yo[z, r : r + 1, :] = functools.reduce(lambda a, b: a + b, vs, yo[z, r : r + 1, :])

    for k in range(2):
        arrived(relays[k])
        arrived(forwards[k])
    for k in range(2):
        for l in range(1, LEVELS):
            n, rows = min(7, BY >> l), wide2.at[l - 1, k]
            rows[pl.ds(0, n, stride=1 << l), :] = down2[k, :n]
            last = pl.ds(BY - (6 << l), 6, stride=1 << l)
            rows[last, :] = rows[last, :] + up2[k, 10:]
        wide2[2, k, 0:1] = wide2[2, k, 0:1] + down3[k, 6:7]
    w, r = lanes_of((8, BX)), lax.broadcasted_iota(jnp.int32, (8, BX), 0)
    top = jnp.where(w % 8 < 4, down2[0, 8:], down2[1, 8:])
    low = jnp.where(w % 8 < 4, up2[0, :8], up2[1, :8])
    ends = jnp.where(r < 4, top, low)
    not_lower = jnp.logical_or(r % 2 == 1, w % 2 == 1)
    for z in range(NZ):
        tiles = [yo[z, 8 * i : 8 * i + 8, :] for i in range(6)]
        e = spread(0, z, ends, None, None, not_lower if z % 2 == 0 else None)
        tiles[0] = tiles[0] + jnp.where(r < 4, e, 0.0)
        tiles[5] = tiles[5] + jnp.where(r < 4, 0.0, e)
        for l in range(1, LEVELS):
            if z % (1 << l):
                continue
            p = z >> l
            for i in (0, 1, 4, 5) if l == 1 else range(6):
                keep = w % (1 << l) == 0
                if p % 2 == 0 and l < LEVELS - 1:
                    keep = jnp.logical_and(keep, jnp.logical_or(r % (2 << l) > 0, w % (2 << l) > 0))
                a, b = (wide2[l - 1, k, 8 * i : 8 * i + 8, :] for k in range(2))
                tiles[i] = tiles[i] + spread(l, p, None, a, b, keep)
        out_ref[z] = jnp.concatenate(tiles, axis=0).astype(BF16)

    for to, _, c in sum(own_far + relays + forwards, farcopies + xcopies + y1copies):
        pl.when(to)(c.wait_send)


def body(quantized, scales):
    groups, tiles = lax.axis_size("grp"), lax.axis_size("tile")
    hbm = pl.BlockSpec(memory_space=pl.ANY)
    dma = pltpu.SemaphoreType.DMA
    return pl.pallas_call(
        functools.partial(kernel, groups, tiles),
        out_shape=pltpu.VMEM((NZ, BY, BX), BF16),
        in_specs=[hbm] * 5,

        scratch_shapes=[
            pltpu.VMEM((NZ, BY, BX), BF16),
            pltpu.VMEM((1, NZ, BY), F32),
            pltpu.VMEM((LEVELS, 2 * BX, 2 * BX), BF16),
            pltpu.VMEM((LEVELS, BY + 16, 3 * BY), BF16),
            pltpu.VMEM((LEVELS - 1, 40, 3 * BY), BF16),
            pltpu.VMEM((NP, BY, BX), BF16),
            pltpu.VMEM((NP, BY, BX), BF16),
            *[pltpu.VMEM((BY, BX), F32) for _ in range(4)],
            *[pltpu.VMEM((24, BX), F32) for _ in range(4)],
            pltpu.VMEM((LEVELS, 2, BY, BX), F32),
            pltpu.VMEM((LEVELS - 1, 2, BY, BX), F32),
            pltpu.VMEM((NP, BY, BX), F32),
            pltpu.VMEM((2, NZ, 4, BX), F32),
            pltpu.VMEM((2, 6, 8, BX), F32),
            pltpu.VMEM((2, NZ, 4, BX), F32),
            pltpu.VMEM((2, 6, 8, BX), F32),
            pltpu.VMEM((8, BX), F32),
            pltpu.VMEM((2, 16, BX), F32),
            pltpu.VMEM((2, 16, BX), F32),
            pltpu.VMEM((2, 8, BX), F32),
            pltpu.VMEM((2, 16, BX), F32),
            pltpu.VMEM((2, 16, BX), F32),
            pltpu.VMEM((2, 8, BX), F32),
            dma((5,)), dma((4,)), dma((4,)), dma((11,)), dma((11,)), dma((12,)), dma((6,)),
        ],
        compiler_params=pltpu.CompilerParams(collective_id=0, has_side_effects=True),
    )(quantized, scales, jnp.asarray(x_matrices()), jnp.asarray(y_matrices(groups)),
      jnp.asarray(packed_matrices(groups)))


def solution(mesh):
    return jax.shard_map(
        body,
        mesh=mesh,
        in_specs=(P(None, "grp", "tile"), P("tile", None, "grp")),
        out_specs=P(None, "grp", "tile"),
        check_vma=False,
    )
```

```python
import functools

import jax
import jax.numpy as jnp
import numpy as np
from jax import lax
from jax.experimental import pallas as pl
from jax.experimental.pallas import tpu as pltpu
from jax.sharding import PartitionSpec as P

LEVELS = 4
ALPHA = -1.586134342059924
BETA = -0.052980118572961
GAMMA = 0.882911075530934
DELTA = 0.443506852043971
KAPPA = 1.230174104914001

NZ, BY, BX = 16, 48, 128
OFF = (0, 16, 24, 28)
NP = 30
SR = (0, 0, 1, 3)
SL = (0, 1, 2, 0)
SLOT = (0, 0, 4, 5)
MESH = pl.DeviceIdType.MESH
F32, BF16 = jnp.float32, jnp.bfloat16


def lift_list(v):
    e, o = list(v[0::2]), list(v[1::2])
    m = len(e)
    up = lambda s: [s[min(i + 1, m - 1)] for i in range(m)]
    down = lambda s: [s[max(i - 1, 0)] for i in range(m)]
    o = [x + ALPHA * (a + b) for x, a, b in zip(o, e, up(e))]
    e = [x + BETA * (a + b) for x, a, b in zip(e, down(o), o)]
    o = [x + GAMMA * (a + b) for x, a, b in zip(o, e, up(e))]
    e = [x + DELTA * (a + b) for x, a, b in zip(e, down(o), o)]
    e = [x * (1.0 / KAPPA) for x in e]
    o = [x * (KAPPA / 2.0) for x in o]
    return [x for pair in zip(e, o) for x in pair]


def level_matrices(n):
    low, out = np.eye(n), []
    for _ in range(LEVELS):
        full = np.stack(lift_list(list(low)))
        out.append(full)
        low = full[::2]
    return out


def split(a):
    hi = a.astype(np.float32).astype(BF16)
    lo = (a - hi.astype(np.float64)).astype(np.float32).astype(BF16)
    return hi, lo


def hi_hi_lo(a):
    hi, lo = split(a)
    return np.concatenate([hi, hi, lo], axis=-1)


@functools.cache
def x_matrices():
    w = level_matrices(3 * BX)
    m = np.zeros((3, LEVELS, BX, 2 * BX))
    for v in range(3):
        for l in range(LEVELS):
            b, win = BX >> l, 8 << l
            mine = w[l][:, v * BX : (v + 1) * BX]
            for j in range(b):
                m[v, l, :, j << l] = mine[v * b + j]
            for start in range(0, BX, win):
                if v < 2:
                    for j in range(4 if l == 0 else 7):
                        lane = start + (j << l) + SR[l]
                        if j << l < win:
                            m[v, l, :, BX + lane] = mine[(v + 1) * b + j]
                if v > 0:
                    for j in range(1, 5 if l == 0 else 7):
                        lane = (start - (j << l) + SL[l]) % BX
                        m[v, l, :, BX + lane] = mine[v * b - j]
    hi, lo = split(m)
    return np.concatenate([hi, lo], axis=2)


@functools.cache
def y_matrices(groups):
    n = groups * BY
    w = level_matrices(n)
    m = np.zeros((groups, LEVELS, BY + 16, BY))
    for g in range(groups):
        for l in range(LEVELS):
            b = BY >> l
            mine = w[l][:, g * BY : (g + 1) * BY]
            for j in range(b):
                m[g, l, j << l] = mine[g * b + j]
            for k in range(8):
                r = (g + 1) * b + k
                if r < n >> l:
                    m[g, l, BY + k] = mine[r]
                r = g * b - 8 + k
                if r >= max((g - 1) * b, 0):
                    m[g, l, BY + 8 + k] = mine[r]
    return hi_hi_lo(m)


@functools.cache
def packed_matrices(groups):
    m = y_matrices(groups)
    out = np.zeros((groups, LEVELS - 1, 40, 3 * BY), m.dtype)
    for l in range(1, LEVELS):
        out[:, l - 1, : BY >> l] = m[:, l, : BY : 1 << l]
        out[:, l - 1, 24:] = m[:, l, BY:]
    return out


def hilo(x):
    hi = x.astype(BF16)
    return hi, (x - hi.astype(F32)).astype(BF16)


def stacked(x):
    hi, lo = hilo(x)
    return jnp.concatenate([hi, lo, hi], axis=0)


def dot(a, b):
    return jnp.dot(a, b, preferred_element_type=F32)


def lanes_of(shape):
    return lax.broadcasted_iota(jnp.int32, shape, len(shape) - 1)


def spread(l, p, packed0, packed_r, packed_l, keep=None):
    win = 8 << l
    turned = lambda e, s: pltpu.roll(e, (-s) % BX, 1)
    both = (lambda m: m) if keep is None else (lambda m: jnp.logical_and(m, keep))
    if l == 0:
        return jnp.where(both((lanes_of(packed0.shape) + 4) % BX < 8), turned(packed0, 8 * p), 0.0)
    w = lanes_of(packed_r.shape)
    a = jnp.where(both(w < win), turned(packed_r, win * p + SR[l]), 0.0)
    return a + jnp.where(both(w >= BX - win), turned(packed_l, win * p + SL[l]), 0.0)


def kernel(
    groups, tiles,
    q_hbm, s_hbm, mx_hbm, ay_hbm, ac_hbm, yo, down2, up2, down3,
    qv, sv, mxv, ayv, acv, zh, zl, to_right, to_left, from_left, from_right,
    to_right_far, to_left_far, from_left_far, from_right_far, wide, own_y,
    send0, send1, recv0, recv1, recv2,
    pass_down, pass_up, pass_down2,
    load_sem, xs_sem, xr_sem, ys_sem, yr_sem, ps_sem, pr_sem,
):
    g, t = lax.axis_index("grp"), lax.axis_index("tile")
    right, left = lax.rem(t + 1, tiles), lax.rem(t + tiles - 1, tiles)
    below, above = lax.rem(g + 1, groups), lax.rem(g + groups - 1, groups)
    below2, above2 = lax.rem(g + 2, groups), lax.rem(g + groups - 2, groups)

    has_left, has_right = t > 0, t < tiles - 1
    has_above, has_below = g > 0, g < groups - 1
    has_above2, has_below2 = g > 1, g < groups - 2
    odd = lax.rem(t, 2) == 1
    even = jnp.logical_not(odd)
    also = lambda *conditions: functools.reduce(jnp.logical_and, conditions)
    barrier = pltpu.get_barrier_semaphore()
    for there, dev in (
        (has_left, (g, left)), (has_right, (g, right)),
        (has_above, (above, t)), (has_below, (below, t)),
        (has_above2, (above2, t)), (has_below2, (below2, t)),
    ):
        @pl.when(there)
        def _():
            pl.semaphore_signal(barrier, inc=1, device_id=dev, device_id_type=MESH)

    side = jnp.where(t == 0, 0, jnp.where(t == tiles - 1, 2, 1))
    loads = [
        pltpu.make_async_copy(q_hbm, qv, load_sem.at[0]),
        pltpu.make_async_copy(s_hbm, sv, load_sem.at[1]),
        pltpu.make_async_copy(mx_hbm.at[side], mxv, load_sem.at[2]),
        pltpu.make_async_copy(ay_hbm.at[g], ayv, load_sem.at[3]),
        pltpu.make_async_copy(ac_hbm.at[g], acv, load_sem.at[4]),
    ]
    for c in loads:
        c.start()
    for there, buffers in (
        (has_left, (from_left, from_left_far)),
        (has_right, (from_right, from_right_far)),
        (has_above, (recv0.at[0], recv1.at[0], down2)),
        (has_below, (recv0.at[1], recv1.at[1], up2)),
        (has_above2, (recv2, down3)),
        (jnp.logical_or(odd, has_left), (down2.at[0], up2.at[0], down3.at[0])),
    ):
        @pl.when(jnp.logical_not(there))
        def _():
            for b in buffers:
                b[...] = jnp.zeros(b.shape, F32)
    loads[1].wait()
    loads[0].wait()

    st = jnp.transpose(sv[0])
    for c in range(3):
        rows = slice(16 * c, 16 * c + 16)
        band = [qv[z, rows, :].astype(F32) * st[rows, z : z + 1] for z in range(NZ)]
        for l in range(LEVELS):
            band = lift_list(band)
            for p, v in enumerate(band):
                hi, lo = hilo(v)
                zh[OFF[l] + p, rows, :] = hi
                zl[OFF[l] + p, rows, :] = lo
            band = band[0::2]

    loads[2].wait()
    own, packs = [], []
    lane = lanes_of((1, 1, BX))
    for l in range(LEVELS):
        n, win = NZ >> l, 8 << l
        h = zh[OFF[l] : OFF[l] + n].reshape(n * BY, BX)
        low = zl[OFF[l] : OFF[l] + n].reshape(n * BY, BX)
        mh, ml = mxv[l, :BX], mxv[l, BX:]
        r = dot(jnp.concatenate([h, low, h], axis=1), jnp.concatenate([mh, mh, ml], axis=0))
        own.append(r[:, :BX].reshape(n, BY, BX))
        if l == 0:
            plane = ((lane + 4) // 8) % NZ
        else:
            rightward = (lane % (1 << l)) == SR[l] % (1 << l)
            plane = jnp.where(rightward, lane // win, (lane // win + 1) % n)
        which = lax.broadcasted_iota(jnp.int32, (n, 1, BX), 0)
        packs.append(jnp.sum(jnp.where(which == plane, r[:, BX:].reshape(n, BY, BX), 0.0), axis=0))

    loads[3].wait()
    loads[4].wait()
    e0 = dot(ayv[0], stacked(packs[0]))
    e1, e2, e3 = (dot(acv[l - 1], stacked(packs[l])) for l in range(1, LEVELS))
    lane = lanes_of((40, BX))
    rightward = jnp.where(lane % 2 == 0, e1, jnp.where(lane % 4 == 1, e2, e3))
    leftward = jnp.where(lane % 2 == 1, e1, jnp.where(lane % 4 == 2, e2, e3))
    for far, v in ((to_right_far, rightward), (to_left_far, leftward)):
        far[:8] = v[24:32]
        far[8:16] = e0[48:56] + e0[56:]
        far[16:] = v[32:]
    lane = lanes_of((24, BX))
    to_right[:24] = jnp.where(lane % 8 < 4, e0[:24], pltpu.roll(e0[24:48], 4, 1))
    to_left[:24] = jnp.where(lane % 8 >= 4, e0[:24], pltpu.roll(e0[24:48], BX - 4, 1))
    to_right[24:] = rightward[:24]
    to_left[24:] = leftward[:24]
    lane = lanes_of((BY, BX))

    def remote(src, dst, ss, rs, dev):
        return pltpu.make_async_remote_copy(
            src_ref=src, dst_ref=dst, send_sem=ss, recv_sem=rs, device_id=dev, device_id_type=MESH
        )

    def start(copies):
        for to, _, c in copies:
            pl.when(to)(c.start)

    def arrived(copies):
        for _, came, c in copies:
            pl.when(came)(c.wait_recv)

    neighbours = (
        jnp.where(has_left, 1, 0) + jnp.where(has_right, 1, 0) + jnp.where(has_above, 1, 0)
        + jnp.where(has_below, 1, 0) + jnp.where(has_above2, 1, 0) + jnp.where(has_below2, 1, 0)
    )
    pl.semaphore_wait(barrier, neighbours)
    farcopies = [
        (also(even, has_right), also(odd, has_left), remote(to_right_far, from_left_far, xs_sem.at[0], xr_sem.at[0], (g, right))),
        (also(even, has_left), also(odd, has_right), remote(to_left_far, from_right_far, xs_sem.at[1], xr_sem.at[1], (g, left))),
    ]

    def along_y(k, far, down, up, down_2, send, recv, first):
        return [
            (also(odd, has_below), also(odd, has_above), remote(far.at[:16], down.at[k], send.at[first + k], recv.at[first + k], (below, t))),
            (also(odd, has_above), also(odd, has_below), remote(far.at[8:], up.at[k], send.at[first + 2 + k], recv.at[first + 2 + k], (above, t))),
            (also(odd, has_below2), also(odd, has_above2), remote(far.at[:8], down_2.at[k], send.at[first + 4 + k], recv.at[first + 4 + k], (below2, t))),
        ]

    own_far = [along_y(k, far, pass_down, pass_up, pass_down2, ps_sem, pr_sem, 0) for k, far in enumerate((to_right_far, to_left_far))]
    relays = [along_y(k, far, down2, up2, down3, ys_sem, yr_sem, 5) for k, far in enumerate((from_left_far, from_right_far))]
    forwards = []
    for k, to, came, dev in ((0, has_right, has_left, (g, right)), (1, has_left, has_right, (g, left))):
        forwards.append([
            (also(odd, to, there), also(even, came, there), remote(src.at[k], dst.at[k], ps_sem.at[6 + 2 * i + k], yr_sem.at[5 + 2 * i + k], dev))
            for i, (there, src, dst) in enumerate(((has_above, pass_down, down2), (has_below, pass_up, up2), (has_above2, pass_down2, down3)))
        ])
    start(own_far[0])
    start(own_far[1])
    start(farcopies)
    xcopies = [
        (has_right, has_left, remote(to_right, from_left, xs_sem.at[2], xr_sem.at[2], (g, right))),
        (has_left, has_right, remote(to_left, from_right, xs_sem.at[3], xr_sem.at[3], (g, left))),
    ]
    start(xcopies)

    for l in range(LEVELS):
        n = NZ >> l
        r = dot(ayv[l], stacked(jnp.concatenate([own[l][p] for p in range(n)], axis=1)))
        tail = [r[BY:, p * BX : (p + 1) * BX] for p in range(n)]
        for p in range(n):
            own_y[OFF[l] + p] = r[:BY, p * BX : (p + 1) * BX]
            if l == 0:
                send0[0, p] = tail[p][:4]
                send0[1, p] = tail[p][12:]
        for first in range(0, n, 1 << l) if l else ():
            both = tail[first]
            for p in range(first + 1, min(first + (1 << l), n)):
                both = both + pltpu.roll(tail[p], p - first, 1)
            send1[0, SLOT[l] + (first >> l)] = both[:8]
            send1[1, SLOT[l] + (first >> l)] = both[8:]
    y1copies = [
        (has_below, has_above, remote(send0.at[0], recv0.at[0], ys_sem.at[0], yr_sem.at[0], (below, t))),
        (has_above, has_below, remote(send0.at[1], recv0.at[1], ys_sem.at[1], yr_sem.at[1], (above, t))),
        (has_below, has_above, remote(send1.at[0], recv1.at[0], ys_sem.at[2], yr_sem.at[2], (below, t))),
        (has_above, has_below, remote(send1.at[1], recv1.at[1], ys_sem.at[3], yr_sem.at[3], (above, t))),
        (has_below2, has_above2, remote(send1.at[0, SLOT[3]], recv2, ys_sem.at[4], yr_sem.at[4], (below2, t))),
    ]
    start(y1copies)

    arrived(farcopies[:1])
    start(relays[0])
    arrived(own_far[0])
    start(forwards[0])
    arrived(own_far[1])
    start(forwards[1])
    arrived(farcopies[1:])
    start(relays[1])

    arrived(xcopies)
    a, b = from_left[:24], from_right[:24]
    w = lanes_of((24, BX)) % 8 < 4
    wide[0, 0, :24] = jnp.where(w, a, b)
    wide[0, 0, 24:] = jnp.where(w, pltpu.roll(a, BX - 4, 1), pltpu.roll(b, 4, 1))
    for l in range(1, LEVELS):
        n = BY >> l
        wide[l, 0, pl.ds(0, n, stride=1 << l), :] = from_left[24 : 24 + n]
        wide[l, 1, pl.ds(0, n, stride=1 << l), :] = from_right[24 : 24 + n]

    row = lax.broadcasted_iota(jnp.int32, (BY, BX), 0)
    for z in range(NZ):
        value = None
        for l in reversed(range(LEVELS)):
            if z % (1 << l):
                continue
            p = z >> l
            part = own_y[OFF[l] + p] + spread(l, p, wide[l, 0], wide[l, 0], wide[l, 1])
            if value is None:
                value = part
            else:
                step = 2 << l
                value = jnp.where((row % step == 0) & (lane % step == 0), value, part)
        yo[z] = value

    arrived(y1copies)
    lane = lanes_of((1, BX))

    def valid(l, p, j, v):
        if l and p % 2 == 0 and j % 2 == 0 and l < LEVELS - 1:
            return jnp.where(lane % (2 << l) == 1 << l, v, 0.0)
        if l:
            return jnp.where(lane % (1 << l) == 0, v, 0.0)
        if p % 2 == 0 and j % 2 == 0:
            return jnp.where(lane % 2 == 1, v, 0.0)
        return v

    for z in range(NZ):
        adds = {}
        for l in range(LEVELS):
            if z % (1 << l):
                continue
            p = z >> l
            if l == 0:
                down, up = recv0[0, p], recv0[1, p]
            else:
                slot, turn = SLOT[l] + (p >> l), (BX - p % (1 << l)) % BX
                down = pltpu.roll(recv1[0, slot], turn, 1)
                up = pltpu.roll(recv1[1, slot], turn, 1)
            for k in range(3 if l == 0 else 7):
                if k << l < BY:
                    adds.setdefault(k << l, []).append(valid(l, p, k, down[k : k + 1]))
            for k in range(4 if l == 0 else 2, 8):
                adds.setdefault(BY - ((8 - k) << l), []).append(valid(l, p, k, up[k - 4 : k - 3] if l == 0 else up[k : k + 1]))
            if l == 3:
                v = pltpu.roll(recv2[...], turn, 1)
                adds[0].append(valid(l, p, 6, v[6:7]))
        for r, vs in adds.items():
            yo[z, r : r + 1, :] = functools.reduce(lambda a, b: a + b, vs, yo[z, r : r + 1, :])

    for to, _, c in sum(own_far + relays + forwards, farcopies + xcopies + y1copies):
        pl.when(to)(c.wait_send)
    for k in range(2):
        arrived(relays[k])
        arrived(forwards[k])


def last_kernel(yo, down2, up2, down3, out_hbm, wide2, rounded, sem):
    wide2[...] = jnp.zeros(wide2.shape, F32)
    for k in range(2):
        for l in range(1, LEVELS):
            n, rows = min(7, BY >> l), wide2.at[l - 1, k]
            rows[pl.ds(0, n, stride=1 << l), :] = down2[k, :n]
            last = pl.ds(BY - (6 << l), 6, stride=1 << l)
            rows[last, :] = rows[last, :] + up2[k, 10:]
        wide2[2, k, 0:1] = wide2[2, k, 0:1] + down3[k, 6:7]
    w, r = lanes_of((8, BX)), lax.broadcasted_iota(jnp.int32, (8, BX), 0)
    top = jnp.where(w % 8 < 4, down2[0, 8:], down2[1, 8:])
    low = jnp.where(w % 8 < 4, up2[0, :8], up2[1, :8])
    ends = jnp.where(r < 4, top, low)
    not_lower = jnp.logical_or(r % 2 == 1, w % 2 == 1)
    for z in (*range(1, NZ, 2), *range(0, NZ, 2)):
        tiles = [yo[z, 8 * i : 8 * i + 8, :] for i in range(6)]
        e = spread(0, z, ends, None, None, not_lower if z % 2 == 0 else None)
        tiles[0] = tiles[0] + jnp.where(r < 4, e, 0.0)
        tiles[5] = tiles[5] + jnp.where(r < 4, 0.0, e)
        for l in range(1, LEVELS):
            if z % (1 << l):
                continue
            p = z >> l
            for i in (0, 1, 4, 5) if l == 1 else range(6):
                keep = w % (1 << l) == 0
                if p % 2 == 0 and l < LEVELS - 1:
                    keep = jnp.logical_and(keep, jnp.logical_or(r % (2 << l) > 0, w % (2 << l) > 0))
                a, b = (wide2[l - 1, k, 8 * i : 8 * i + 8, :] for k in range(2))
                tiles[i] = tiles[i] + spread(l, p, None, a, b, keep)
        rounded[z] = jnp.concatenate(tiles, axis=0).astype(BF16)
        pltpu.make_async_copy(rounded.at[z], out_hbm.at[z], sem.at[0]).start()
    pltpu.make_async_copy(rounded, out_hbm, sem.at[0]).wait()


def body(quantized, scales):
    groups, tiles = lax.axis_size("grp"), lax.axis_size("tile")
    hbm = pl.BlockSpec(memory_space=pl.ANY)
    dma = pltpu.SemaphoreType.DMA
    held = pl.pallas_call(
        functools.partial(kernel, groups, tiles),
        out_shape=[
            pltpu.VMEM((NZ, BY, BX), F32),
            pltpu.VMEM((2, 16, BX), F32),
            pltpu.VMEM((2, 16, BX), F32),
            pltpu.VMEM((2, 8, BX), F32),
        ],
        in_specs=[hbm] * 5,

        scratch_shapes=[
            pltpu.VMEM((NZ, BY, BX), BF16),
            pltpu.VMEM((1, NZ, BY), F32),
            pltpu.VMEM((LEVELS, 2 * BX, 2 * BX), BF16),
            pltpu.VMEM((LEVELS, BY + 16, 3 * BY), BF16),
            pltpu.VMEM((LEVELS - 1, 40, 3 * BY), BF16),
            pltpu.VMEM((NP, BY, BX), BF16),
            pltpu.VMEM((NP, BY, BX), BF16),
            *[pltpu.VMEM((BY, BX), F32) for _ in range(4)],
            *[pltpu.VMEM((24, BX), F32) for _ in range(4)],
            pltpu.VMEM((LEVELS, 2, BY, BX), F32),
            pltpu.VMEM((NP, BY, BX), F32),
            pltpu.VMEM((2, NZ, 4, BX), F32),
            pltpu.VMEM((2, 6, 8, BX), F32),
            pltpu.VMEM((2, NZ, 4, BX), F32),
            pltpu.VMEM((2, 6, 8, BX), F32),
            pltpu.VMEM((8, BX), F32),
            pltpu.VMEM((2, 16, BX), F32),
            pltpu.VMEM((2, 16, BX), F32),
            pltpu.VMEM((2, 8, BX), F32),
            dma((5,)), dma((4,)), dma((4,)), dma((11,)), dma((11,)), dma((12,)), dma((6,)),
        ],
        compiler_params=pltpu.CompilerParams(collective_id=0, has_side_effects=True),
    )(quantized, scales, jnp.asarray(x_matrices()), jnp.asarray(y_matrices(groups)),
      jnp.asarray(packed_matrices(groups)))
    return pl.pallas_call(
        last_kernel,
        out_shape=jax.ShapeDtypeStruct((NZ, BY, BX), BF16),
        in_specs=[pl.BlockSpec(memory_space=pltpu.VMEM)] * 4,
        out_specs=hbm,
        scratch_shapes=[
            pltpu.VMEM((LEVELS - 1, 2, BY, BX), F32),
            pltpu.VMEM((NZ, BY, BX), BF16),
            dma((1,)),
        ],
        compiler_params=pltpu.CompilerParams(vmem_limit_bytes=8 << 20),
    )(*held)


def solution(mesh):
    return jax.shard_map(
        body,
        mesh=mesh,
        in_specs=(P(None, "grp", "tile"), P("tile", None, "grp")),
        out_specs=P(None, "grp", "tile"),
        check_vma=False,
    )
```

```python
import functools

import jax
import jax.numpy as jnp
import numpy as np
from jax import lax
from jax.experimental import pallas as pl
from jax.experimental.pallas import tpu as pltpu
from jax.sharding import PartitionSpec as P

LEVELS = 4
ALPHA = -1.586134342059924
BETA = -0.052980118572961
GAMMA = 0.882911075530934
DELTA = 0.443506852043971
KAPPA = 1.230174104914001

NZ, BY, BX = 16, 48, 128
OFF = (0, 16, 24, 28)
NP = 30
SR = (0, 0, 1, 3)
SL = (0, 1, 2, 0)
SLOT = (0, 0, 4, 5)
MESH = pl.DeviceIdType.MESH
F32, BF16 = jnp.float32, jnp.bfloat16


def lift_list(v):
    e, o = list(v[0::2]), list(v[1::2])
    m = len(e)
    up = lambda s: [s[min(i + 1, m - 1)] for i in range(m)]
    down = lambda s: [s[max(i - 1, 0)] for i in range(m)]
    o = [x + ALPHA * (a + b) for x, a, b in zip(o, e, up(e))]
    e = [x + BETA * (a + b) for x, a, b in zip(e, down(o), o)]
    o = [x + GAMMA * (a + b) for x, a, b in zip(o, e, up(e))]
    e = [x + DELTA * (a + b) for x, a, b in zip(e, down(o), o)]
    e = [x * (1.0 / KAPPA) for x in e]
    o = [x * (KAPPA / 2.0) for x in o]
    return [x for pair in zip(e, o) for x in pair]


def level_matrices(n):
    low, out = np.eye(n), []
    for _ in range(LEVELS):
        full = np.stack(lift_list(list(low)))
        out.append(full)
        low = full[::2]
    return out


def split(a):
    hi = a.astype(np.float32).astype(BF16)
    lo = (a - hi.astype(np.float64)).astype(np.float32).astype(BF16)
    return hi, lo


def hi_hi_lo(a):
    hi, lo = split(a)
    return np.concatenate([hi, hi, lo], axis=-1)


@functools.cache
def x_matrices():
    w = level_matrices(3 * BX)
    m = np.zeros((3, LEVELS, BX, 2 * BX))
    for v in range(3):
        for l in range(LEVELS):
            b, win = BX >> l, 8 << l
            mine = w[l][:, v * BX : (v + 1) * BX]
            for j in range(b):
                m[v, l, :, j << l] = mine[v * b + j]
            for start in range(0, BX, win):
                if v < 2:
                    for j in range(4 if l == 0 else 7):
                        lane = start + (j << l) + SR[l]
                        if j << l < win:
                            m[v, l, :, BX + lane] = mine[(v + 1) * b + j]
                if v > 0:
                    for j in range(1, 5 if l == 0 else 7):
                        lane = (start - (j << l) + SL[l]) % BX
                        m[v, l, :, BX + lane] = mine[v * b - j]
    hi, lo = split(m)
    return np.concatenate([hi, lo], axis=2)


@functools.cache
def y_matrices(groups):
    n = groups * BY
    w = level_matrices(n)
    m = np.zeros((groups, LEVELS, BY + 16, BY))
    for g in range(groups):
        for l in range(LEVELS):
            b = BY >> l
            mine = w[l][:, g * BY : (g + 1) * BY]
            for j in range(b):
                m[g, l, j << l] = mine[g * b + j]
            for k in range(8):
                r = (g + 1) * b + k
                if r < n >> l:
                    m[g, l, BY + k] = mine[r]
                r = g * b - 8 + k
                if r >= max((g - 1) * b, 0):
                    m[g, l, BY + 8 + k] = mine[r]
    return hi_hi_lo(m)


@functools.cache
def packed_matrices(groups):
    m = y_matrices(groups)
    out = np.zeros((groups, LEVELS - 1, 40, 3 * BY), m.dtype)
    for l in range(1, LEVELS):
        out[:, l - 1, : BY >> l] = m[:, l, : BY : 1 << l]
        out[:, l - 1, 24:] = m[:, l, BY:]
    return out


def hilo(x):
    hi = x.astype(BF16)
    return hi, (x - hi.astype(F32)).astype(BF16)


def stacked(x):
    hi, lo = hilo(x)
    return jnp.concatenate([hi, lo, hi], axis=0)


def dot(a, b):
    return jnp.dot(a, b, preferred_element_type=F32)


def lanes_of(shape):
    return lax.broadcasted_iota(jnp.int32, shape, len(shape) - 1)


def spread(l, p, packed0, packed_r, packed_l, keep=None):
    win = 8 << l
    turned = lambda e, s: pltpu.roll(e, (-s) % BX, 1)
    both = (lambda m: m) if keep is None else (lambda m: jnp.logical_and(m, keep))
    if l == 0:
        return jnp.where(both((lanes_of(packed0.shape) + 4) % BX < 8), turned(packed0, 8 * p), 0.0)
    w = lanes_of(packed_r.shape)
    a = jnp.where(both(w < win), turned(packed_r, win * p + SR[l]), 0.0)
    return a + jnp.where(both(w >= BX - win), turned(packed_l, win * p + SL[l]), 0.0)


def kernel(
    groups, tiles,
    q_hbm, s_hbm, mx_hbm, ay_hbm, ac_hbm, yo, down2, up2, down3,
    qv, sv, mxv, ayv, acv, zh, zl, to_right, to_left, from_left, from_right,
    to_right_far, to_left_far, wide, own_y,
    send0, send1, recv0, recv1, recv2,
    pass_down, pass_up, pass_down2, far3,
    load_sem, xs_sem, xr_sem, ys_sem, yr_sem, ps_sem, pr_sem, ready,
):
    g, t = lax.axis_index("grp"), lax.axis_index("tile")
    right, left = lax.rem(t + 1, tiles), lax.rem(t + tiles - 1, tiles)
    below, above = lax.rem(g + 1, groups), lax.rem(g + groups - 1, groups)
    below2, above2 = lax.rem(g + 2, groups), lax.rem(g + groups - 2, groups)

    has_left, has_right = t > 0, t < tiles - 1
    has_above, has_below = g > 0, g < groups - 1
    has_above2, has_below2 = g > 1, g < groups - 2
    odd = lax.rem(t, 2) == 1
    even = jnp.logical_not(odd)
    also = lambda *conditions: functools.reduce(jnp.logical_and, conditions)
    half = groups // 2
    jump = jnp.logical_and(g >= half - 2, g < half)
    landed = jnp.logical_and(g >= half, g < half + 2)
    barrier = pltpu.get_barrier_semaphore()
    for there, dev in (
        (has_left, (g, left)), (also(odd, has_right), (g, right)),
        (has_above, (above, t)), (has_below, (below, t)),
        (has_above2, (above2, t)), (has_below2, (below2, t)),
        *(
            (also(odd, to, there), (y, x))
            for to, x in ((has_left, left), (has_right, right))
            for there, y in ((has_above, above), (has_below, below), (landed, above2))
        ),
    ):
        @pl.when(there)
        def _():
            pl.semaphore_signal(barrier, inc=1, device_id=dev, device_id_type=MESH)

    side = jnp.where(t == 0, 0, jnp.where(t == tiles - 1, 2, 1))
    matrices = [
        pltpu.make_async_copy(mx_hbm.at[side, l], mxv.at[l], load_sem.at[4 + l]) for l in range(LEVELS)
    ]
    loads = [
        pltpu.make_async_copy(q_hbm, qv, load_sem.at[0]),
        pltpu.make_async_copy(s_hbm, sv, load_sem.at[1]),
        pltpu.make_async_copy(ay_hbm.at[g], ayv, load_sem.at[2]),
        pltpu.make_async_copy(ac_hbm.at[g], acv, load_sem.at[3]),
    ]
    for c in loads[:2] + matrices + loads[2:]:
        c.start()
    for there, buffers in (
        (has_left, (from_left, down2.at[0], up2.at[0], down3.at[0])),
        (has_right, (from_right, down2.at[1], up2.at[1], down3.at[1])),
        (has_above, (recv0.at[0], recv1.at[0], down2)),
        (has_below, (recv0.at[1], recv1.at[1], up2)),
        (has_above2, (recv2, down3)),
    ):
        @pl.when(jnp.logical_not(there))
        def _():
            for b in buffers:
                b[...] = jnp.zeros(b.shape, F32)
    loads[1].wait()
    loads[0].wait()

    st = jnp.transpose(sv[0])
    for c in range(3):
        rows = slice(16 * c, 16 * c + 16)
        band = [qv[z, rows, :].astype(F32) * st[rows, z : z + 1] for z in range(NZ)]
        for l in range(LEVELS):
            band = lift_list(band)
            for p, v in enumerate(band):
                hi, lo = hilo(v)
                zh[OFF[l] + p, rows, :] = hi
                zl[OFF[l] + p, rows, :] = lo
            band = band[0::2]

    for c in matrices + loads[2:]:
        c.wait()
    own, packs = [], []
    lane = lanes_of((1, 1, BX))
    for l in range(LEVELS):
        n, win = NZ >> l, 8 << l
        h = zh[OFF[l] : OFF[l] + n].reshape(n * BY, BX)
        low = zl[OFF[l] : OFF[l] + n].reshape(n * BY, BX)
        mh, ml = mxv[l, :BX], mxv[l, BX:]
        r = dot(jnp.concatenate([h, low, h], axis=1), jnp.concatenate([mh, mh, ml], axis=0))
        own.append(r[:, :BX].reshape(n, BY, BX))
        if l == 0:
            plane = ((lane + 4) // 8) % NZ
        else:
            rightward = (lane % (1 << l)) == SR[l] % (1 << l)
            plane = jnp.where(rightward, lane // win, (lane // win + 1) % n)
        which = lax.broadcasted_iota(jnp.int32, (n, 1, BX), 0)
        packs.append(jnp.sum(jnp.where(which == plane, r[:, BX:].reshape(n, BY, BX), 0.0), axis=0))

    e0 = dot(ayv[0], stacked(packs[0]))
    e1, e2, e3 = (dot(acv[l - 1], stacked(packs[l])) for l in range(1, LEVELS))
    lane = lanes_of((40, BX))
    rightward = jnp.where(lane % 2 == 0, e1, jnp.where(lane % 4 == 1, e2, e3))
    leftward = jnp.where(lane % 2 == 1, e1, jnp.where(lane % 4 == 2, e2, e3))
    for far, v in ((to_right_far, rightward), (to_left_far, leftward)):
        far[:8] = v[24:32]
        far[8:16] = e0[48:56] + e0[56:]
        far[16:] = v[32:]
    lane = lanes_of((24, BX))
    to_right[:24] = jnp.where(lane % 8 < 4, e0[:24], pltpu.roll(e0[24:48], 4, 1))
    to_left[:24] = jnp.where(lane % 8 >= 4, e0[:24], pltpu.roll(e0[24:48], BX - 4, 1))
    to_right[24:] = rightward[:24]
    to_left[24:] = leftward[:24]
    lane = lanes_of((BY, BX))

    def remote(src, dst, ss, rs, dev):
        return pltpu.make_async_remote_copy(
            src_ref=src, dst_ref=dst, send_sem=ss, recv_sem=rs, device_id=dev, device_id_type=MESH
        )

    def start(copies):
        for to, _, c in copies:
            pl.when(to)(c.start)

    def arrived(copies):
        for _, came, c in copies:
            pl.when(came)(c.wait_recv)

    one = lambda condition: jnp.where(condition, 1, 0)
    sides = one(has_left) + one(has_right)
    along = one(has_above) + one(has_below) + one(has_above2) + one(has_below2)
    across = sides * (1 + one(has_above) + one(has_below) + one(jump))
    pl.semaphore_wait(barrier, along + jnp.where(even, across, one(has_right)))

    @pl.when(even)
    def _():
        pl.semaphore_signal(ready, inc=1, device_id=(g, right), device_id_type=MESH)

    straight, second, relays = [], [], []
    near2 = also(has_below2, jnp.logical_not(jump))
    for k, far, to, came, x in (
        (0, to_right_far, has_right, has_left, right), (1, to_left_far, has_left, has_right, left)
    ):
        straight += [
            (also(even, to, has_below), also(odd, came, has_above), remote(far.at[:16], down2.at[k], ys_sem.at[5 + k], yr_sem.at[5 + k], (below, x))),
            (also(even, to, has_above), also(odd, came, has_below), remote(far.at[8:], up2.at[k], ys_sem.at[7 + k], yr_sem.at[7 + k], (above, x))),
            (also(even, to, jump), also(odd, came, landed), remote(far.at[:8], down3.at[k], ys_sem.at[9 + k], yr_sem.at[9 + k], (below2, x))),
        ]
        second.append((also(even, to, near2), also(odd, came, near2), remote(far.at[:8], far3.at[k], xs_sem.at[2 + k], xr_sem.at[2 + k], (g, x))))
        relays.append((also(odd, came, near2), also(odd, came, has_above2, jnp.logical_not(landed)), remote(far3.at[k], down3.at[k], ys_sem.at[9 + k], yr_sem.at[9 + k], (below2, t))))

    def along_y(k, far, down, up, down_2, send, recv, first):
        return [
            (also(odd, has_below), also(odd, has_above), remote(far.at[:16], down.at[k], send.at[first + k], recv.at[first + k], (below, t))),
            (also(odd, has_above), also(odd, has_below), remote(far.at[8:], up.at[k], send.at[first + 2 + k], recv.at[first + 2 + k], (above, t))),
            (also(odd, has_below2), also(odd, has_above2), remote(far.at[:8], down_2.at[k], send.at[first + 4 + k], recv.at[first + 4 + k], (below2, t))),
        ]

    own_far = [along_y(k, far, pass_down, pass_up, pass_down2, ps_sem, pr_sem, 0) for k, far in enumerate((to_right_far, to_left_far))]
    forwards = []
    for k, to, came, dev in ((0, has_right, has_left, (g, right)), (1, has_left, has_right, (g, left))):
        forwards.append([
            (also(odd, to, there), also(even, came, there), remote(src.at[k], dst.at[k], ps_sem.at[6 + 2 * i + k], yr_sem.at[5 + 2 * i + k], dev))
            for i, (there, src, dst) in enumerate(((has_above, pass_down, down2), (has_below, pass_up, up2), (has_above2, pass_down2, down3)))
        ])
    start(own_far[0])
    start(own_far[1])
    start(straight)
    start(second)
    xcopies = [
        (has_right, has_left, remote(to_right, from_left, xs_sem.at[0], xr_sem.at[0], (g, right))),
        (has_left, has_right, remote(to_left, from_right, xs_sem.at[1], xr_sem.at[1], (g, left))),
    ]
    start([xcopies[0], (also(even, has_left), has_right, xcopies[1][2])])

    for l in range(LEVELS):
        n = NZ >> l
        r = dot(ayv[l], stacked(jnp.concatenate([own[l][p] for p in range(n)], axis=1)))
        tail = [r[BY:, p * BX : (p + 1) * BX] for p in range(n)]
        for p in range(n):
            own_y[OFF[l] + p] = r[:BY, p * BX : (p + 1) * BX]
            if l == 0:
                send0[0, p] = tail[p][:4]
                send0[1, p] = tail[p][12:]
        for first in range(0, n, 1 << l) if l else ():
            both = tail[first]
            for p in range(first + 1, min(first + (1 << l), n)):
                both = both + pltpu.roll(tail[p], p - first, 1)
            send1[0, SLOT[l] + (first >> l)] = both[:8]
            send1[1, SLOT[l] + (first >> l)] = both[8:]
    y1copies = [
        (has_below, has_above, remote(send0.at[0], recv0.at[0], ys_sem.at[0], yr_sem.at[0], (below, t))),
        (has_above, has_below, remote(send0.at[1], recv0.at[1], ys_sem.at[1], yr_sem.at[1], (above, t))),
        (has_below, has_above, remote(send1.at[0], recv1.at[0], ys_sem.at[2], yr_sem.at[2], (below, t))),
        (has_above, has_below, remote(send1.at[1], recv1.at[1], ys_sem.at[3], yr_sem.at[3], (above, t))),
        (has_below2, has_above2, remote(send1.at[0, SLOT[3]], recv2, ys_sem.at[4], yr_sem.at[4], (below2, t))),
    ]
    start(y1copies)

    arrived(own_far[0])
    start(forwards[0])
    arrived(second[1:])
    start(relays[1:])

    @pl.when(odd)
    def _():
        pl.semaphore_wait(ready, 1)
        xcopies[1][2].start()

    arrived(own_far[1])
    start(forwards[1])
    arrived(second[:1])
    start(relays[:1])

    arrived(xcopies)
    a, b = from_left[:24], from_right[:24]
    w = lanes_of((24, BX)) % 8 < 4
    wide[0, 0, :24] = jnp.where(w, a, b)
    wide[0, 0, 24:] = jnp.where(w, pltpu.roll(a, BX - 4, 1), pltpu.roll(b, 4, 1))
    for l in range(1, LEVELS):
        n = BY >> l
        wide[l, 0, pl.ds(0, n, stride=1 << l), :] = from_left[24 : 24 + n]
        wide[l, 1, pl.ds(0, n, stride=1 << l), :] = from_right[24 : 24 + n]

    row = lax.broadcasted_iota(jnp.int32, (BY, BX), 0)
    for z in range(NZ):
        value = None
        for l in reversed(range(LEVELS)):
            if z % (1 << l):
                continue
            p = z >> l
            part = own_y[OFF[l] + p] + spread(l, p, wide[l, 0], wide[l, 0], wide[l, 1])
            if value is None:
                value = part
            else:
                step = 2 << l
                value = jnp.where((row % step == 0) & (lane % step == 0), value, part)
        yo[z] = value

    arrived(y1copies)
    lane = lanes_of((1, BX))

    def valid(l, p, j, v):
        if l and p % 2 == 0 and j % 2 == 0 and l < LEVELS - 1:
            return jnp.where(lane % (2 << l) == 1 << l, v, 0.0)
        if l:
            return jnp.where(lane % (1 << l) == 0, v, 0.0)
        if p % 2 == 0 and j % 2 == 0:
            return jnp.where(lane % 2 == 1, v, 0.0)
        return v

    for z in range(NZ):
        adds = {}
        for l in range(LEVELS):
            if z % (1 << l):
                continue
            p = z >> l
            if l == 0:
                down, up = recv0[0, p], recv0[1, p]
            else:
                slot, turn = SLOT[l] + (p >> l), (BX - p % (1 << l)) % BX
                down = pltpu.roll(recv1[0, slot], turn, 1)
                up = pltpu.roll(recv1[1, slot], turn, 1)
            for k in range(3 if l == 0 else 7):
                if k << l < BY:
                    adds.setdefault(k << l, []).append(valid(l, p, k, down[k : k + 1]))
            for k in range(4 if l == 0 else 2, 8):
                adds.setdefault(BY - ((8 - k) << l), []).append(valid(l, p, k, up[k - 4 : k - 3] if l == 0 else up[k : k + 1]))
            if l == 3:
                v = pltpu.roll(recv2[...], turn, 1)
                adds[0].append(valid(l, p, 6, v[6:7]))
        for r, vs in adds.items():
            yo[z, r : r + 1, :] = functools.reduce(lambda a, b: a + b, vs, yo[z, r : r + 1, :])

    for to, _, c in sum(own_far + forwards, straight + second + relays + xcopies + y1copies):
        pl.when(to)(c.wait_send)
    arrived(straight)
    arrived(relays)
    for k in range(2):
        arrived(forwards[k])


def last_kernel(yo, down2, up2, down3, out_hbm, wide2, rounded, sem):
    wide2[...] = jnp.zeros(wide2.shape, F32)
    for k in range(2):
        for l in range(1, LEVELS):
            n, rows = min(7, BY >> l), wide2.at[l - 1, k]
            rows[pl.ds(0, n, stride=1 << l), :] = down2[k, :n]
            last = pl.ds(BY - (6 << l), 6, stride=1 << l)
            rows[last, :] = rows[last, :] + up2[k, 10:]
        wide2[2, k, 0:1] = wide2[2, k, 0:1] + down3[k, 6:7]
    w, r = lanes_of((8, BX)), lax.broadcasted_iota(jnp.int32, (8, BX), 0)
    top = jnp.where(w % 8 < 4, down2[0, 8:], down2[1, 8:])
    low = jnp.where(w % 8 < 4, up2[0, :8], up2[1, :8])
    ends = jnp.where(r < 4, top, low)
    not_lower = jnp.logical_or(r % 2 == 1, w % 2 == 1)
    for z in (*range(1, NZ, 2), *range(0, NZ, 2)):
        tiles = [yo[z, 8 * i : 8 * i + 8, :] for i in range(6)]
        e = spread(0, z, ends, None, None, not_lower if z % 2 == 0 else None)
        tiles[0] = tiles[0] + jnp.where(r < 4, e, 0.0)
        tiles[5] = tiles[5] + jnp.where(r < 4, 0.0, e)
        for l in range(1, LEVELS):
            if z % (1 << l):
                continue
            p = z >> l
            for i in (0, 1, 4, 5) if l == 1 else range(6):
                keep = w % (1 << l) == 0
                if p % 2 == 0 and l < LEVELS - 1:
                    keep = jnp.logical_and(keep, jnp.logical_or(r % (2 << l) > 0, w % (2 << l) > 0))
                a, b = (wide2[l - 1, k, 8 * i : 8 * i + 8, :] for k in range(2))
                tiles[i] = tiles[i] + spread(l, p, None, a, b, keep)
        rounded[z] = jnp.concatenate(tiles, axis=0).astype(BF16)
        pltpu.make_async_copy(rounded.at[z], out_hbm.at[z], sem.at[0]).start()
    pltpu.make_async_copy(rounded, out_hbm, sem.at[0]).wait()


def body(quantized, scales):
    groups, tiles = lax.axis_size("grp"), lax.axis_size("tile")
    hbm = pl.BlockSpec(memory_space=pl.ANY)
    dma = pltpu.SemaphoreType.DMA
    held = pl.pallas_call(
        functools.partial(kernel, groups, tiles),
        out_shape=[
            pltpu.VMEM((NZ, BY, BX), F32),
            pltpu.VMEM((2, 16, BX), F32),
            pltpu.VMEM((2, 16, BX), F32),
            pltpu.VMEM((2, 8, BX), F32),
        ],
        in_specs=[hbm] * 5,

        scratch_shapes=[
            pltpu.VMEM((NZ, BY, BX), BF16),
            pltpu.VMEM((1, NZ, BY), F32),
            pltpu.VMEM((LEVELS, 2 * BX, 2 * BX), BF16),
            pltpu.VMEM((LEVELS, BY + 16, 3 * BY), BF16),
            pltpu.VMEM((LEVELS - 1, 40, 3 * BY), BF16),
            pltpu.VMEM((NP, BY, BX), BF16),
            pltpu.VMEM((NP, BY, BX), BF16),
            *[pltpu.VMEM((BY, BX), F32) for _ in range(4)],
            *[pltpu.VMEM((24, BX), F32) for _ in range(2)],
            pltpu.VMEM((LEVELS, 2, BY, BX), F32),
            pltpu.VMEM((NP, BY, BX), F32),
            pltpu.VMEM((2, NZ, 4, BX), F32),
            pltpu.VMEM((2, 6, 8, BX), F32),
            pltpu.VMEM((2, NZ, 4, BX), F32),
            pltpu.VMEM((2, 6, 8, BX), F32),
            pltpu.VMEM((8, BX), F32),
            pltpu.VMEM((2, 16, BX), F32),
            pltpu.VMEM((2, 16, BX), F32),
            pltpu.VMEM((2, 8, BX), F32),
            pltpu.VMEM((2, 8, BX), F32),
            dma((8,)), dma((4,)), dma((4,)), dma((11,)), dma((11,)), dma((12,)), dma((6,)),
            pltpu.SemaphoreType.REGULAR,
        ],
        compiler_params=pltpu.CompilerParams(collective_id=0, has_side_effects=True),
    )(quantized, scales, jnp.asarray(x_matrices()), jnp.asarray(y_matrices(groups)),
      jnp.asarray(packed_matrices(groups)))
    return pl.pallas_call(
        last_kernel,
        out_shape=jax.ShapeDtypeStruct((NZ, BY, BX), BF16),
        in_specs=[pl.BlockSpec(memory_space=pltpu.VMEM)] * 4,
        out_specs=hbm,
        scratch_shapes=[
            pltpu.VMEM((LEVELS - 1, 2, BY, BX), F32),
            pltpu.VMEM((NZ, BY, BX), BF16),
            dma((1,)),
        ],
        compiler_params=pltpu.CompilerParams(vmem_limit_bytes=8 << 20),
    )(*held)


def solution(mesh):
    return jax.shard_map(
        body,
        mesh=mesh,
        in_specs=(P(None, "grp", "tile"), P("tile", None, "grp")),
        out_specs=P(None, "grp", "tile"),
        check_vma=False,
    )
```

```python
import functools

import jax
import jax.numpy as jnp
import numpy as np
from jax import lax
from jax.experimental import pallas as pl
from jax.experimental.pallas import tpu as pltpu
from jax.sharding import PartitionSpec as P

LEVELS = 4
ALPHA = -1.586134342059924
BETA = -0.052980118572961
GAMMA = 0.882911075530934
DELTA = 0.443506852043971
KAPPA = 1.230174104914001

NZ, BY, BX = 16, 48, 128
OFF = (0, 16, 24, 28)
NP = 30
SR = (0, 0, 1, 3)
SL = (0, 1, 2, 0)
SLOT = (0, 0, 4, 5)
MESH = pl.DeviceIdType.MESH
F32, BF16 = jnp.float32, jnp.bfloat16


def lift_list(v):
    e, o = list(v[0::2]), list(v[1::2])
    m = len(e)
    up = lambda s: [s[min(i + 1, m - 1)] for i in range(m)]
    down = lambda s: [s[max(i - 1, 0)] for i in range(m)]
    o = [x + ALPHA * (a + b) for x, a, b in zip(o, e, up(e))]
    e = [x + BETA * (a + b) for x, a, b in zip(e, down(o), o)]
    o = [x + GAMMA * (a + b) for x, a, b in zip(o, e, up(e))]
    e = [x + DELTA * (a + b) for x, a, b in zip(e, down(o), o)]
    e = [x * (1.0 / KAPPA) for x in e]
    o = [x * (KAPPA / 2.0) for x in o]
    return [x for pair in zip(e, o) for x in pair]


def level_matrices(n):
    low, out = np.eye(n), []
    for _ in range(LEVELS):
        full = np.stack(lift_list(list(low)))
        out.append(full)
        low = full[::2]
    return out


def split(a):
    hi = a.astype(np.float32).astype(BF16)
    lo = (a - hi.astype(np.float64)).astype(np.float32).astype(BF16)
    return hi, lo


def hi_hi_lo(a):
    hi, lo = split(a)
    return np.concatenate([hi, hi, lo], axis=-1)


@functools.cache
def x_matrices():
    w = level_matrices(3 * BX)
    m = np.zeros((3, LEVELS, BX, 2 * BX))
    for v in range(3):
        for l in range(LEVELS):
            b, win = BX >> l, 8 << l
            mine = w[l][:, v * BX : (v + 1) * BX]
            for j in range(b):
                m[v, l, :, j << l] = mine[v * b + j]
            for start in range(0, BX, win):
                if v < 2:
                    for j in range(4 if l == 0 else 7):
                        lane = start + (j << l) + SR[l]
                        if j << l < win:
                            m[v, l, :, BX + lane] = mine[(v + 1) * b + j]
                if v > 0:
                    for j in range(1, 5 if l == 0 else 7):
                        lane = (start - (j << l) + SL[l]) % BX
                        m[v, l, :, BX + lane] = mine[v * b - j]
    hi, lo = split(m)
    return np.concatenate([hi, lo], axis=2)


@functools.cache
def y_matrices(groups):
    n = groups * BY
    w = level_matrices(n)
    m = np.zeros((groups, LEVELS, BY + 16, BY))
    for g in range(groups):
        for l in range(LEVELS):
            b = BY >> l
            mine = w[l][:, g * BY : (g + 1) * BY]
            for j in range(b):
                m[g, l, j << l] = mine[g * b + j]
            for k in range(8):
                r = (g + 1) * b + k
                if r < n >> l:
                    m[g, l, BY + k] = mine[r]
                r = g * b - 8 + k
                if r >= max((g - 1) * b, 0):
                    m[g, l, BY + 8 + k] = mine[r]
    return hi_hi_lo(m)


@functools.cache
def packed_matrices(groups):
    m = y_matrices(groups)
    out = np.zeros((groups, LEVELS - 1, 40, 3 * BY), m.dtype)
    for l in range(1, LEVELS):
        out[:, l - 1, : BY >> l] = m[:, l, : BY : 1 << l]
        out[:, l - 1, 24:] = m[:, l, BY:]
    return out


def hilo(x):
    hi = x.astype(BF16)
    return hi, (x - hi.astype(F32)).astype(BF16)


def stacked(x):
    hi, lo = hilo(x)
    return jnp.concatenate([hi, lo, hi], axis=0)


def dot(a, b):
    return jnp.dot(a, b, preferred_element_type=F32)


def lanes_of(shape):
    return lax.broadcasted_iota(jnp.int32, shape, len(shape) - 1)


def spread(l, p, packed0, packed_r, packed_l, keep=None):
    win = 8 << l
    turned = lambda e, s: pltpu.roll(e, (-s) % BX, 1)
    both = (lambda m: m) if keep is None else (lambda m: jnp.logical_and(m, keep))
    if l == 0:
        return jnp.where(both((lanes_of(packed0.shape) + 4) % BX < 8), turned(packed0, 8 * p), 0.0)
    w = lanes_of(packed_r.shape)
    a = jnp.where(both(w < win), turned(packed_r, win * p + SR[l]), 0.0)
    return a + jnp.where(both(w >= BX - win), turned(packed_l, win * p + SL[l]), 0.0)


def kernel(
    groups, tiles,
    q_hbm, s_hbm, mx_hbm, ay_hbm, ac_hbm, yo, down2, up2, down3,
    qv, sv, mxv, ayv, acv, zh, zl, to_right, to_left, from_left, from_right,
    to_right_far, to_left_far, wide, own_y,
    send0, send1, recv0, recv1, recv2,
    pass_down, pass_up, pass_down2, far3,
    load_sem, xs_sem, xr_sem, ys_sem, yr_sem, ps_sem, pr_sem, ready,
):
    g, t = lax.axis_index("grp"), lax.axis_index("tile")
    right, left = lax.rem(t + 1, tiles), lax.rem(t + tiles - 1, tiles)
    below, above = lax.rem(g + 1, groups), lax.rem(g + groups - 1, groups)
    below2, above2 = lax.rem(g + 2, groups), lax.rem(g + groups - 2, groups)

    has_left, has_right = t > 0, t < tiles - 1
    has_above, has_below = g > 0, g < groups - 1
    has_above2, has_below2 = g > 1, g < groups - 2
    odd = lax.rem(t, 2) == 1
    even = jnp.logical_not(odd)
    also = lambda *conditions: functools.reduce(jnp.logical_and, conditions)
    half = groups // 2
    jump = jnp.logical_and(g >= half - 2, g < half)
    landed = jnp.logical_and(g >= half, g < half + 2)
    barrier = pltpu.get_barrier_semaphore()
    for there, dev in (
        (has_left, (g, left)), (also(odd, has_right), (g, right)),
        (has_above, (above, t)), (has_below, (below, t)),
        (has_above2, (above2, t)), (has_below2, (below2, t)),
        *(
            (also(odd, to, there), (y, x))
            for to, x in ((has_left, left), (has_right, right))
            for there, y in ((has_above, above), (has_below, below), (landed, above2))
        ),
    ):
        @pl.when(there)
        def _():
            pl.semaphore_signal(barrier, inc=1, device_id=dev, device_id_type=MESH)

    side = jnp.where(t == 0, 0, jnp.where(t == tiles - 1, 2, 1))
    matrices = [
        pltpu.make_async_copy(mx_hbm.at[side, l], mxv.at[l], load_sem.at[4 + l]) for l in range(LEVELS)
    ]
    loads = [
        pltpu.make_async_copy(q_hbm, qv, load_sem.at[0]),
        pltpu.make_async_copy(s_hbm, sv, load_sem.at[1]),
        pltpu.make_async_copy(ay_hbm.at[g], ayv, load_sem.at[2]),
        pltpu.make_async_copy(ac_hbm.at[g], acv, load_sem.at[3]),
    ]
    for c in loads[:2] + matrices + loads[2:]:
        c.start()
    for there, buffers in (
        (has_left, (from_left, down2.at[0], up2.at[0], down3.at[0])),
        (has_right, (from_right, down2.at[1], up2.at[1], down3.at[1])),
        (has_above, (recv0.at[0], recv1.at[0], down2)),
        (has_below, (recv0.at[1], recv1.at[1], up2)),
        (has_above2, (recv2, down3)),
    ):
        @pl.when(jnp.logical_not(there))
        def _():
            for b in buffers:
                b[...] = jnp.zeros(b.shape, F32)
    loads[1].wait()
    loads[0].wait()

    st = jnp.transpose(sv[0])
    for c in range(3):
        rows = slice(16 * c, 16 * c + 16)
        band = [qv[z, rows, :].astype(F32) * st[rows, z : z + 1] for z in range(NZ)]
        for l in range(LEVELS):
            band = lift_list(band)
            for p, v in enumerate(band):
                hi, lo = hilo(v)
                zh[OFF[l] + p, rows, :] = hi
                zl[OFF[l] + p, rows, :] = lo
            band = band[0::2]

    for c in matrices + loads[2:]:
        c.wait()
    own, packs = [], []
    lane = lanes_of((1, 1, BX))
    for l in range(LEVELS):
        n, win = NZ >> l, 8 << l
        h = zh[OFF[l] : OFF[l] + n].reshape(n * BY, BX)
        low = zl[OFF[l] : OFF[l] + n].reshape(n * BY, BX)
        mh, ml = mxv[l, :BX], mxv[l, BX:]
        r = dot(jnp.concatenate([h, low, h], axis=1), jnp.concatenate([mh, mh, ml], axis=0))
        own.append(r[:, :BX].reshape(n, BY, BX))
        if l == 0:
            plane = ((lane + 4) // 8) % NZ
        else:
            rightward = (lane % (1 << l)) == SR[l] % (1 << l)
            plane = jnp.where(rightward, lane // win, (lane // win + 1) % n)
        which = lax.broadcasted_iota(jnp.int32, (n, 1, BX), 0)
        packs.append(jnp.sum(jnp.where(which == plane, r[:, BX:].reshape(n, BY, BX), 0.0), axis=0))

    e0 = dot(ayv[0], stacked(packs[0]))
    e1, e2, e3 = (dot(acv[l - 1], stacked(packs[l])) for l in range(1, LEVELS))
    lane = lanes_of((40, BX))
    rightward = jnp.where(lane % 2 == 0, e1, jnp.where(lane % 4 == 1, e2, e3))
    leftward = jnp.where(lane % 2 == 1, e1, jnp.where(lane % 4 == 2, e2, e3))
    for far, v in ((to_right_far, rightward), (to_left_far, leftward)):
        far[:8] = v[24:32]
        far[8:16] = e0[48:56] + e0[56:]
        far[16:] = v[32:]
    lane = lanes_of((24, BX))
    to_right[:24] = jnp.where(lane % 8 < 4, e0[:24], pltpu.roll(e0[24:48], 4, 1))
    to_left[:24] = jnp.where(lane % 8 >= 4, e0[:24], pltpu.roll(e0[24:48], BX - 4, 1))
    to_right[24:] = rightward[:24]
    to_left[24:] = leftward[:24]
    lane = lanes_of((BY, BX))

    def remote(src, dst, ss, rs, dev):
        return pltpu.make_async_remote_copy(
            src_ref=src, dst_ref=dst, send_sem=ss, recv_sem=rs, device_id=dev, device_id_type=MESH
        )

    def start(copies):
        for to, _, c in copies:
            pl.when(to)(c.start)

    def arrived(copies):
        for _, came, c in copies:
            pl.when(came)(c.wait_recv)

    one = lambda condition: jnp.where(condition, 1, 0)
    sides = one(has_left) + one(has_right)
    along = one(has_above) + one(has_below) + one(has_above2) + one(has_below2)
    across = sides * (1 + one(has_above) + one(has_below) + one(jump))
    pl.semaphore_wait(barrier, along + jnp.where(even, across, one(has_right)))

    @pl.when(even)
    def _():
        pl.semaphore_signal(ready, inc=1, device_id=(g, right), device_id_type=MESH)

    straight, second, relays = [], [], []
    near2 = also(has_below2, jnp.logical_not(jump))
    for k, far, to, came, x in (
        (0, to_right_far, has_right, has_left, right), (1, to_left_far, has_left, has_right, left)
    ):
        straight += [
            (also(even, to, has_below), also(odd, came, has_above), remote(far.at[:16], down2.at[k], ys_sem.at[5 + k], yr_sem.at[5 + k], (below, x))),
            (also(even, to, has_above), also(odd, came, has_below), remote(far.at[8:], up2.at[k], ys_sem.at[7 + k], yr_sem.at[7 + k], (above, x))),
            (also(even, to, jump), also(odd, came, landed), remote(far.at[:8], down3.at[k], ys_sem.at[9 + k], yr_sem.at[9 + k], (below2, x))),
        ]
        second.append((also(even, to, near2), also(odd, came, near2), remote(far.at[:8], far3.at[k], xs_sem.at[2 + k], xr_sem.at[2 + k], (g, x))))
        relays.append((also(odd, came, near2), also(odd, came, has_above2, jnp.logical_not(landed)), remote(far3.at[k], down3.at[k], ys_sem.at[9 + k], yr_sem.at[9 + k], (below2, t))))

    def along_y(k, far, down, up, down_2, send, recv, first):
        return [
            (also(odd, has_below), also(odd, has_above), remote(far.at[:16], down.at[k], send.at[first + k], recv.at[first + k], (below, t))),
            (also(odd, has_above), also(odd, has_below), remote(far.at[8:], up.at[k], send.at[first + 2 + k], recv.at[first + 2 + k], (above, t))),
            (also(odd, has_below2), also(odd, has_above2), remote(far.at[:8], down_2.at[k], send.at[first + 4 + k], recv.at[first + 4 + k], (below2, t))),
        ]

    own_far = [along_y(k, far, pass_down, pass_up, pass_down2, ps_sem, pr_sem, 0) for k, far in enumerate((to_right_far, to_left_far))]
    forwards = []
    for k, to, came, dev in ((0, has_right, has_left, (g, right)), (1, has_left, has_right, (g, left))):
        forwards.append([
            (also(odd, to, there), also(even, came, there), remote(src.at[k], dst.at[k], ps_sem.at[6 + 2 * i + k], yr_sem.at[5 + 2 * i + k], dev))
            for i, (there, src, dst) in enumerate(((has_above, pass_down, down2), (has_below, pass_up, up2), (has_above2, pass_down2, down3)))
        ])
    start(own_far[0])
    start(own_far[1])
    start(straight)
    start(second)
    xcopies = [
        (has_right, has_left, remote(to_right, from_left, xs_sem.at[0], xr_sem.at[0], (g, right))),
        (has_left, has_right, remote(to_left, from_right, xs_sem.at[1], xr_sem.at[1], (g, left))),
    ]
    start([xcopies[0], (also(even, has_left), has_right, xcopies[1][2])])

    for l in range(LEVELS):
        n = NZ >> l
        r = dot(ayv[l], stacked(jnp.concatenate([own[l][p] for p in range(n)], axis=1)))
        tail = [r[BY:, p * BX : (p + 1) * BX] for p in range(n)]
        for p in range(n):
            own_y[OFF[l] + p] = r[:BY, p * BX : (p + 1) * BX]
            if l == 0:
                send0[0, p] = tail[p][:4]
                send0[1, p] = tail[p][12:]
        for first in range(0, n, 1 << l) if l else ():
            both = tail[first]
            for p in range(first + 1, min(first + (1 << l), n)):
                both = both + pltpu.roll(tail[p], p - first, 1)
            send1[0, SLOT[l] + (first >> l)] = both[:8]
            send1[1, SLOT[l] + (first >> l)] = both[8:]
    y1copies = [
        (has_below, has_above, remote(send0.at[0], recv0.at[0], ys_sem.at[0], yr_sem.at[0], (below, t))),
        (has_above, has_below, remote(send0.at[1], recv0.at[1], ys_sem.at[1], yr_sem.at[1], (above, t))),
        (has_below, has_above, remote(send1.at[0], recv1.at[0], ys_sem.at[2], yr_sem.at[2], (below, t))),
        (has_above, has_below, remote(send1.at[1], recv1.at[1], ys_sem.at[3], yr_sem.at[3], (above, t))),
        (has_below2, has_above2, remote(send1.at[0, SLOT[3]], recv2, ys_sem.at[4], yr_sem.at[4], (below2, t))),
    ]
    start(y1copies)

    for came, on in zip(own_far[0], forwards[0]):
        arrived([came])
        start([on])
    arrived(second[1:])
    start(relays[1:])

    @pl.when(odd)
    def _():
        pl.semaphore_wait(ready, 1)
        xcopies[1][2].start()

    for came, on in zip(own_far[1], forwards[1]):
        arrived([came])
        start([on])
    arrived(second[:1])
    start(relays[:1])

    arrived(xcopies)
    a, b = from_left[:24], from_right[:24]
    w = lanes_of((24, BX)) % 8 < 4
    wide[0, 0, :24] = jnp.where(w, a, b)
    wide[0, 0, 24:] = jnp.where(w, pltpu.roll(a, BX - 4, 1), pltpu.roll(b, 4, 1))
    for l in range(1, LEVELS):
        n = BY >> l
        wide[l, 0, pl.ds(0, n, stride=1 << l), :] = from_left[24 : 24 + n]
        wide[l, 1, pl.ds(0, n, stride=1 << l), :] = from_right[24 : 24 + n]

    row = lax.broadcasted_iota(jnp.int32, (BY, BX), 0)
    for z in range(NZ):
        value = None
        for l in reversed(range(LEVELS)):
            if z % (1 << l):
                continue
            p = z >> l
            part = own_y[OFF[l] + p] + spread(l, p, wide[l, 0], wide[l, 0], wide[l, 1])
            if value is None:
                value = part
            else:
                step = 2 << l
                value = jnp.where((row % step == 0) & (lane % step == 0), value, part)
        yo[z] = value

    arrived(y1copies)
    lane = lanes_of((1, BX))

    def valid(l, p, j, v):
        if l and p % 2 == 0 and j % 2 == 0 and l < LEVELS - 1:
            return jnp.where(lane % (2 << l) == 1 << l, v, 0.0)
        if l:
            return jnp.where(lane % (1 << l) == 0, v, 0.0)
        if p % 2 == 0 and j % 2 == 0:
            return jnp.where(lane % 2 == 1, v, 0.0)
        return v

    for z in range(NZ):
        adds = {}
        for l in range(LEVELS):
            if z % (1 << l):
                continue
            p = z >> l
            if l == 0:
                down, up = recv0[0, p], recv0[1, p]
            else:
                slot, turn = SLOT[l] + (p >> l), (BX - p % (1 << l)) % BX
                down = pltpu.roll(recv1[0, slot], turn, 1)
                up = pltpu.roll(recv1[1, slot], turn, 1)
            for k in range(3 if l == 0 else 7):
                if k << l < BY:
                    adds.setdefault(k << l, []).append(valid(l, p, k, down[k : k + 1]))
            for k in range(4 if l == 0 else 2, 8):
                adds.setdefault(BY - ((8 - k) << l), []).append(valid(l, p, k, up[k - 4 : k - 3] if l == 0 else up[k : k + 1]))
            if l == 3:
                v = pltpu.roll(recv2[...], turn, 1)
                adds[0].append(valid(l, p, 6, v[6:7]))
        for r, vs in adds.items():
            yo[z, r : r + 1, :] = functools.reduce(lambda a, b: a + b, vs, yo[z, r : r + 1, :])

    for to, _, c in sum(own_far + forwards, straight + second + relays + xcopies + y1copies):
        pl.when(to)(c.wait_send)
    arrived(straight)
    arrived(relays)
    for k in range(2):
        arrived(forwards[k])


def last_kernel(yo, down2, up2, down3, out_hbm, wide2, rounded, sem):
    wide2[...] = jnp.zeros(wide2.shape, F32)
    for k in range(2):
        for l in range(1, LEVELS):
            n, rows = min(7, BY >> l), wide2.at[l - 1, k]
            rows[pl.ds(0, n, stride=1 << l), :] = down2[k, :n]
            last = pl.ds(BY - (6 << l), 6, stride=1 << l)
            rows[last, :] = rows[last, :] + up2[k, 10:]
        wide2[2, k, 0:1] = wide2[2, k, 0:1] + down3[k, 6:7]
    w, r = lanes_of((8, BX)), lax.broadcasted_iota(jnp.int32, (8, BX), 0)
    top = jnp.where(w % 8 < 4, down2[0, 8:], down2[1, 8:])
    low = jnp.where(w % 8 < 4, up2[0, :8], up2[1, :8])
    ends = jnp.where(r < 4, top, low)
    not_lower = jnp.logical_or(r % 2 == 1, w % 2 == 1)
    for z in (*range(1, NZ, 2), *range(0, NZ, 2)):
        tiles = [yo[z, 8 * i : 8 * i + 8, :] for i in range(6)]
        e = spread(0, z, ends, None, None, not_lower if z % 2 == 0 else None)
        tiles[0] = tiles[0] + jnp.where(r < 4, e, 0.0)
        tiles[5] = tiles[5] + jnp.where(r < 4, 0.0, e)
        for l in range(1, LEVELS):
            if z % (1 << l):
                continue
            p = z >> l
            for i in (0, 1, 4, 5) if l == 1 else range(6):
                keep = w % (1 << l) == 0
                if p % 2 == 0 and l < LEVELS - 1:
                    keep = jnp.logical_and(keep, jnp.logical_or(r % (2 << l) > 0, w % (2 << l) > 0))
                a, b = (wide2[l - 1, k, 8 * i : 8 * i + 8, :] for k in range(2))
                tiles[i] = tiles[i] + spread(l, p, None, a, b, keep)
        rounded[z] = jnp.concatenate(tiles, axis=0).astype(BF16)
        pltpu.make_async_copy(rounded.at[z], out_hbm.at[z], sem.at[0]).start()
    pltpu.make_async_copy(rounded, out_hbm, sem.at[0]).wait()


def body(quantized, scales):
    groups, tiles = lax.axis_size("grp"), lax.axis_size("tile")
    hbm = pl.BlockSpec(memory_space=pl.ANY)
    dma = pltpu.SemaphoreType.DMA
    held = pl.pallas_call(
        functools.partial(kernel, groups, tiles),
        out_shape=[
            pltpu.VMEM((NZ, BY, BX), F32),
            pltpu.VMEM((2, 16, BX), F32),
            pltpu.VMEM((2, 16, BX), F32),
            pltpu.VMEM((2, 8, BX), F32),
        ],
        in_specs=[hbm] * 5,

        scratch_shapes=[
            pltpu.VMEM((NZ, BY, BX), BF16),
            pltpu.VMEM((1, NZ, BY), F32),
            pltpu.VMEM((LEVELS, 2 * BX, 2 * BX), BF16),
            pltpu.VMEM((LEVELS, BY + 16, 3 * BY), BF16),
            pltpu.VMEM((LEVELS - 1, 40, 3 * BY), BF16),
            pltpu.VMEM((NP, BY, BX), BF16),
            pltpu.VMEM((NP, BY, BX), BF16),
            *[pltpu.VMEM((BY, BX), F32) for _ in range(4)],
            *[pltpu.VMEM((24, BX), F32) for _ in range(2)],
            pltpu.VMEM((LEVELS, 2, BY, BX), F32),
            pltpu.VMEM((NP, BY, BX), F32),
            pltpu.VMEM((2, NZ, 4, BX), F32),
            pltpu.VMEM((2, 6, 8, BX), F32),
            pltpu.VMEM((2, NZ, 4, BX), F32),
            pltpu.VMEM((2, 6, 8, BX), F32),
            pltpu.VMEM((8, BX), F32),
            pltpu.VMEM((2, 16, BX), F32),
            pltpu.VMEM((2, 16, BX), F32),
            pltpu.VMEM((2, 8, BX), F32),
            pltpu.VMEM((2, 8, BX), F32),
            dma((8,)), dma((4,)), dma((4,)), dma((11,)), dma((11,)), dma((12,)), dma((6,)),
            pltpu.SemaphoreType.REGULAR,
        ],
        compiler_params=pltpu.CompilerParams(collective_id=0, has_side_effects=True),
    )(quantized, scales, jnp.asarray(x_matrices()), jnp.asarray(y_matrices(groups)),
      jnp.asarray(packed_matrices(groups)))
    return pl.pallas_call(
        last_kernel,
        out_shape=jax.ShapeDtypeStruct((NZ, BY, BX), BF16),
        in_specs=[pl.BlockSpec(memory_space=pltpu.VMEM)] * 4,
        out_specs=hbm,
        scratch_shapes=[
            pltpu.VMEM((LEVELS - 1, 2, BY, BX), F32),
            pltpu.VMEM((NZ, BY, BX), BF16),
            dma((1,)),
        ],
        compiler_params=pltpu.CompilerParams(vmem_limit_bytes=8 << 20),
    )(*held)


def solution(mesh):
    return jax.shard_map(
        body,
        mesh=mesh,
        in_specs=(P(None, "grp", "tile"), P("tile", None, "grp")),
        out_specs=P(None, "grp", "tile"),
        check_vma=False,
    )
```
